128 devices in a mesh: gx: 4 (over x), gy: 32 (over z, y, core).
Axes of the slice: x: 4, y: 4, z: 4, core: 2. Of those that a mesh axis runs over, the one named last changes fastest.
Arguments:
- source_values: bfloat16 [16384, 64, 128], P(('gx', 'gy')), may hold values from -6 to 6
- leaf_maps: bfloat16 [16384, 32, 128], P(('gx', 'gy')), may hold values from -0.5 to 0.5
- source_transfers: bfloat16 [4, 16384, 32, 128], P(None, ('gx', 'gy')), may hold values from -0.5 to 0.5
- target_transfers: bfloat16 [4, 16384, 32, 128], P(None, ('gx', 'gy')), may hold values from -0.5 to 0.5
Outputs:
- target_coeffs: bfloat16 [16384, 32, 128], P(('gx', 'gy'))
The draws below stay inside these ranges and needn't reach their ends.
All inputs are finite; a program needn't handle non-finite values.
Results may differ from the reference program's by a relative error of at most 0.012.
Values may be sent and summed in bfloat16 or wider, within the bound.
A program may use at most 128 MiB of HBM per device.

```python
import jax
import jax.numpy as jnp
from jax import lax

RANK = 32
RHS = 64
LEAF = 64
BOX_DEV = 128
LEV = 4
COLS = 128
BOXES = 16384
N_GX = 4
N_GY = 32


def block_scale(rng, shape, shards, smallest, top_value):
    def one(position, parts):
        steps = jax.random.uniform(jax.random.fold_in(jax.random.fold_in(rng, 6), position), (parts,), jnp.float32, smallest / len(shards), top_value / len(shards))
        return jnp.repeat(jnp.exp(steps), shape[position] // parts).reshape((-1,) + (1,) * (len(shape) - position - 1))

    factor_of = one(*shards[0])
    for cut in shards[1:]:
        factor_of = factor_of * one(*cut)
    return factor_of


def bell_draw(own_key, extent, scale, limit, cuts=(), held_as=jnp.bfloat16):
    drawn = jax.random.normal(own_key, extent, jnp.float32) * scale
    if len(cuts) > 0:
        drawn = block_scale(own_key, extent, cuts, -0.22, 0.18) * drawn
    return jnp.clip(drawn, min=-limit, max=limit).astype(held_as)


def setup_inputs(seed: int = 0) -> dict:
    key_list = jax.random.split(jax.random.key(seed), 5)
    source_values = bell_draw(key_list[0], (BOXES, LEAF, COLS), 1.0, 6.0, ((0, 128),))
    leaf_maps = bell_draw(key_list[1], (BOXES, RANK, 2 * LEAF), (2 * LEAF) ** -0.5, 0.5, ((0, 128),))
    source_transfers = bell_draw(key_list[2], (LEV, BOXES, RANK, 4 * RANK), (4 * RANK) ** -0.5, 0.5, ((1, 128),))
    target_transfers = bell_draw(key_list[3], (LEV, BOXES, RANK, 4 * RANK), (4 * RANK) ** -0.5, 0.5, ((1, 128),))
    return {"source_values": source_values, "leaf_maps": leaf_maps, "source_transfers": source_transfers, "target_transfers": target_transfers}


def combine(product):
    nboxes, _, rank_n, cols = product.shape
    pieces = product.reshape(nboxes, 2, rank_n, cols // (2 * RHS), 2, RHS)
    real_part = pieces[:, 0, :, :, 0] - pieces[:, 1, :, :, 1]
    imag_part = pieces[:, 0, :, :, 1] + pieces[:, 1, :, :, 0]
    return jnp.stack([real_part, imag_part], axis=3).reshape(nboxes, rank_n, cols).astype(jnp.bfloat16)


def leaf_step(operands):
    maps_block, values_block = operands
    nboxes, rank_n, width = maps_block.shape
    split = maps_block.reshape(nboxes, rank_n, 2, width // 2).astype(jnp.float32)
    product = jnp.einsum('bipj,bjc->bpic', split, values_block.astype(jnp.float32))
    return combine(product)


def transfer_step(operands):
    coeffs, partner, transfer = operands
    nboxes, rank_n, cols = coeffs.shape
    stacked = jnp.stack([coeffs, partner], axis=1).astype(jnp.float32)
    blocks = transfer.reshape(nboxes, rank_n, 2, 2, rank_n).astype(jnp.float32)
    return combine(jnp.einsum('bispj,bsjc->bpic', blocks, stacked))


def partner_of(coeffs, device_bit):
    span = BOX_DEV * (2 ** device_bit)
    grouped = coeffs.reshape((coeffs.shape[0] // (2 * span), 2, span) + coeffs.shape[1:])
    return grouped[:, ::-1].reshape(coeffs.shape)


def blocked(array):
    devices_n = N_GX * N_GY
    return array.reshape((devices_n, BOX_DEV) + array.shape[1:])


def apply_level(coeffs, transfer, device_bit):
    partner = partner_of(coeffs, device_bit)
    result = lax.map(transfer_step, (blocked(coeffs), blocked(partner), blocked(transfer)))
    return result.reshape(coeffs.shape)


def reference(source_values, leaf_maps, source_transfers, target_transfers):
    devices_n = N_GX * N_GY
    all_bits = devices_n.bit_length() - 1
    coeffs = lax.map(leaf_step, (blocked(leaf_maps), blocked(source_values)))
    coeffs = coeffs.reshape(BOXES, RANK, COLS)
    for level_no in range(LEV):
        coeffs = apply_level(coeffs, source_transfers[level_no], level_no % all_bits)
    piece = BOX_DEV // devices_n
    coeffs = coeffs.reshape(devices_n, devices_n, piece, RANK, COLS).transpose(1, 0, 2, 3, 4).reshape(BOXES, RANK, COLS)
    for level_no in range(LEV):
        coeffs = apply_level(coeffs, target_transfers[level_no], (all_bits - 1 - level_no) % all_bits)
    return coeffs
```

```python
import functools

import jax
import jax.numpy as jnp
from jax import lax
from jax.experimental import pallas as pl
from jax.experimental.pallas import tpu as pltpu
from jax.sharding import PartitionSpec as P

MESH = pl.DeviceIdType.MESH
BF16 = jnp.bfloat16
F32 = jnp.float32


def turned(x):
    wide = pltpu.roll(x.astype(F32), 64, x.ndim - 1)
    lane = lax.broadcasted_iota(jnp.int32, wide.shape, wide.ndim - 1)
    return jnp.where(lane < 64, -wide, wide).astype(BF16)


def dot(a, b):
    return jnp.dot(a, b, preferred_element_type=F32).astype(BF16)


def mixed(own, partner, transfer):
    operand = jnp.concatenate([own, turned(own), partner, turned(partner)], axis=0)
    return dot(transfer, operand)


def mixed_pair(a, b, transfer_a, transfer_b):
    ta, tb = turned(a), turned(b)
    out_a = dot(transfer_a, jnp.concatenate([a, ta, b, tb], axis=0))
    out_b = dot(transfer_b, jnp.concatenate([b, tb, a, ta], axis=0))
    return out_a, out_b


def kernel(
    src, leaf, st, tt, out,
    src_v, leaf_v, s0, sb, tb, c0, c0p, c1, cb, ya, yb, zp, wa, wb,
    load_sem, own_sem, s_send, s_recv, t_send, t_recv, p_send, p_recv,
    y_send, y_recv, z_send, z_recv, r_send, r_recv,
):
    x = lax.axis_index("gx")
    g = lax.axis_index("gy")
    z = g // 8
    yc = g % 8
    core = g % 2
    xz = x * 4 + z

    def at_xz(i, j):
        to_x, to_z = (x + i) % 4, (z + j) % 4
        return (to_x, to_z * 8 + yc), to_x * 4 + to_z

    def at_yc(r):
        to = (yc + r) % 8
        return (x, z * 8 + to), to

    xz_offsets = [(i, j) for i in range(4) for j in range(4) if (i, j) != (0, 0)]
    yc_offsets = list(range(1, 8))
    core_mate = (x, g + 1 - 2 * core)
    z_mate = (x, (z + 1 - 2 * (z % 2)) * 8 + yc)

    loads = [
        pltpu.make_async_copy(src, src_v, load_sem.at[0]),
        pltpu.make_async_copy(leaf, leaf_v, load_sem.at[1]),
        pltpu.make_async_copy(st.at[0], s0, load_sem.at[2]),
    ]
    for copy in loads:
        copy.start()
    own_copies = [pltpu.make_async_copy(tt.at[:, xz], tb.at[:, xz], own_sem.at[3])]
    for level in range(3):
        own_copies.append(
            pltpu.make_async_copy(st.at[level + 1, :, yc], sb.at[level, yc], own_sem.at[level])
        )

    barrier = pltpu.get_barrier_semaphore()
    for i, j in xz_offsets:
        pl.semaphore_signal(barrier, inc=1, device_id=at_xz(i, j)[0], device_id_type=MESH)
    for r in yc_offsets:
        pl.semaphore_signal(barrier, inc=1, device_id=at_yc(r)[0], device_id_type=MESH)
    pl.semaphore_wait(barrier, len(xz_offsets) + len(yc_offsets))

    def s_copy(level, r):
        device, to = at_yc(r)
        return pltpu.make_async_remote_copy(
            src_ref=st.at[level + 1, :, to],
            dst_ref=sb.at[level, yc],
            send_sem=s_send.at[level, r],
            recv_sem=s_recv.at[level, r],
            device_id=device,
            device_id_type=MESH,
        )

    def t_copy(k):
        device, to = at_xz(*xz_offsets[k])
        return pltpu.make_async_remote_copy(
            src_ref=tt.at[:, to],
            dst_ref=tb.at[:, xz],
            send_sem=t_send.at[k],
            recv_sem=t_recv.at[k],
            device_id=device,
            device_id_type=MESH,
        )

    for r in yc_offsets:
        s_copy(0, r).start()
    for k in range(15):
        t_copy(k).start()
    for copy in own_copies:
        copy.start()

    def p_copy(q):
        return pltpu.make_async_remote_copy(
            src_ref=c0.at[pl.ds(4 * q, 4)],
            dst_ref=c0p.at[pl.ds(4 * q, 4)],
            send_sem=p_send.at[q],
            recv_sem=p_recv.at[q],
            device_id=core_mate,
            device_id_type=MESH,
        )

    loads[0].wait()
    loads[1].wait()
    for q in range(4):
        def leaf_body(n, carry, q=q):
            a = 4 * q + n
            for b in range(8):
                v = src_v[a, b]
                c0[a, b] = dot(leaf_v[a, b], jnp.concatenate([v, turned(v)], axis=0))
            return carry

        lax.fori_loop(0, 4, leaf_body, 0)
        p_copy(q).start()

    def y_copy(q, r):
        device, to = at_yc(r)
        return pltpu.make_async_remote_copy(
            src_ref=c1.at[to, pl.ds(4 * q, 4)],
            dst_ref=cb.at[yc, pl.ds(4 * q, 4)],
            send_sem=y_send.at[q, r],
            recv_sem=y_recv.at[q, r],
            device_id=device,
            device_id_type=MESH,
        )

    loads[2].wait()
    for q in range(4):
        p_copy(q).wait_recv()

        def first_body(n, carry, q=q):
            a = 4 * q + n
            for b in range(8):
                c1[b, a] = mixed(c0[a, b], c0p[a, b], s0[a, b])
            return carry

        lax.fori_loop(0, 4, first_body, 0)
        for r in yc_offsets:
            y_copy(q, r).start()
    for level in (1, 2):
        for r in yc_offsets:
            s_copy(level, r).start()
    cb[yc] = c1[yc]

    def y_level(q, bit, level, source, target):
        def body(n, carry):
            a = 4 * q + n
            for b in range(8):
                if b & bit == 0:
                    out_a, out_b = mixed_pair(
                        source[b, a], source[b | bit, a], sb[level, b, a], sb[level, b | bit, a]
                    )
                    target[b, a] = out_a
                    target[b | bit, a] = out_b
            return carry

        lax.fori_loop(0, 4, body, 0)

    for r in yc_offsets:
        s_copy(0, r).wait_recv()
    own_copies[1].wait()
    for q in range(4):
        for r in yc_offsets:
            y_copy(q, r).wait_recv()
        y_level(q, 2, 0, cb, ya)
    for r in yc_offsets:
        s_copy(1, r).wait_recv()
    own_copies[2].wait()
    for q in range(4):
        y_level(q, 4, 1, ya, yb)

    def z_copy(q):
        return pltpu.make_async_remote_copy(
            src_ref=yb.at[pl.ds(2 * q, 2)],
            dst_ref=zp.at[pl.ds(2 * q, 2)],
            send_sem=z_send.at[q],
            recv_sem=z_recv.at[q],
            device_id=z_mate,
            device_id_type=MESH,
        )

    for q in range(4):
        z_copy(q).start()
    for r in yc_offsets:
        s_copy(2, r).wait_recv()
    own_copies[3].wait()
    for k in range(15):
        t_copy(k).wait_recv()
    own_copies[0].wait()

    def r_copy(q, k):
        device, to = at_xz(*xz_offsets[k])
        return pltpu.make_async_remote_copy(
            src_ref=wa.at[pl.ds(2 * q, 2), to],
            dst_ref=out.at[xz, pl.ds(2 * q, 2)],
            send_sem=r_send.at[q, k],
            recv_sem=r_recv.at[q, k],
            device_id=device,
            device_id_type=MESH,
        )

    def last_body(q, carry):
        z_copy(q).wait_recv()
        for h in range(2):
            b = 2 * q + h
            for a in range(16):
                wa[b, a] = mixed(yb[b, a], zp[b, a], sb[2, b, a])
            source, target = wa, wb
            for level, bit in enumerate((8, 4, 2, 1)):
                for a in range(16):
                    if a & bit == 0:
                        out_a, out_b = mixed_pair(
                            source[b, a], source[b, a | bit], tb[level, a, b], tb[level, a | bit, b]
                        )
                        target[b, a] = out_a
                        target[b, a | bit] = out_b
                source, target = target, source
            out[xz, b] = wa[b, xz]
        for k in range(15):
            r_copy(q, k).start()
        return carry

    lax.fori_loop(0, 4, last_body, 0)

    for q in range(4):
        for k in range(15):
            r_copy(q, k).wait()
        p_copy(q).wait_send()
        z_copy(q).wait_send()
        for r in yc_offsets:
            y_copy(q, r).wait_send()
    for level in range(3):
        for r in yc_offsets:
            s_copy(level, r).wait_send()
    for k in range(15):
        t_copy(k).wait_send()


def local(source_values, leaf_maps, source_transfers, target_transfers):
    dma = pltpu.SemaphoreType.DMA
    boxes = (32, 128)
    out = pl.pallas_call(
        kernel,
        out_shape=jax.ShapeDtypeStruct((16, 8) + boxes, BF16),
        in_specs=[pl.BlockSpec(memory_space=pl.ANY)] * 4,
        out_specs=pl.BlockSpec(memory_space=pltpu.VMEM),
        scratch_shapes=[
            pltpu.VMEM((16, 8, 64, 128), BF16),
            pltpu.VMEM((16, 8) + boxes, BF16),
            pltpu.VMEM((16, 8) + boxes, BF16),
            pltpu.VMEM((3, 8, 16) + boxes, BF16),
            pltpu.VMEM((4, 16, 8) + boxes, BF16),
            pltpu.VMEM((16, 8) + boxes, BF16),
            pltpu.VMEM((16, 8) + boxes, BF16),
            pltpu.VMEM((8, 16) + boxes, BF16),
            pltpu.VMEM((8, 16) + boxes, BF16),
            pltpu.VMEM((8, 16) + boxes, BF16),
            pltpu.VMEM((8, 16) + boxes, BF16),
            pltpu.VMEM((8, 16) + boxes, BF16),
            pltpu.VMEM((8, 16) + boxes, BF16),
            pltpu.VMEM((8, 16) + boxes, BF16),
            dma((3,)),
            dma((4,)),
            dma((3, 8)),
            dma((3, 8)),
            dma((15,)),
            dma((15,)),
            dma((4,)),
            dma((4,)),
            dma((4, 8)),
            dma((4, 8)),
            dma((4,)),
            dma((4,)),
            dma((4, 15)),
            dma((4, 15)),
        ],
        compiler_params=pltpu.CompilerParams(
            collective_id=0, has_side_effects=True, vmem_limit_bytes=67_043_328
        ),
    )(
        source_values.reshape(16, 8, 64, 128),
        leaf_maps.reshape((16, 8) + boxes),
        source_transfers.reshape((4, 16, 8) + boxes),
        target_transfers.reshape((4, 16, 8) + boxes),
    )
    return out.reshape((128,) + boxes)


def solution(mesh):
    return jax.shard_map(
        local,
        mesh=mesh,
        in_specs=(
            P(("gx", "gy"), None, None),
            P(("gx", "gy"), None, None),
            P(None, ("gx", "gy"), None, None),
            P(None, ("gx", "gy"), None, None),
        ),
        out_specs=P(("gx", "gy"), None, None),
        check_vma=False,
    )
```

```python
import jax
import jax.numpy as jnp
from jax import lax
from jax.experimental import pallas as pl
from jax.experimental.pallas import tpu as pltpu
from jax.sharding import PartitionSpec as P

MESH = pl.DeviceIdType.MESH
BF16 = jnp.bfloat16
F32 = jnp.float32


def turned(x):
    wide = pltpu.roll(x.astype(F32), 64, x.ndim - 1)
    lane = lax.broadcasted_iota(jnp.int32, wide.shape, wide.ndim - 1)
    return jnp.where(lane < 64, -wide, wide).astype(BF16)


def dot(a, b):
    return jnp.dot(a, b, preferred_element_type=F32).astype(BF16)


def mixed(own, partner, transfer):
    operand = jnp.concatenate([own, turned(own), partner, turned(partner)], axis=0)
    return dot(transfer, operand)


def mixed_pair(a, b, transfer_a, transfer_b):
    ta, tb = turned(a), turned(b)
    out_a = dot(transfer_a, jnp.concatenate([a, ta, b, tb], axis=0))
    out_b = dot(transfer_b, jnp.concatenate([b, tb, a, ta], axis=0))
    return out_a, out_b


def paired(values, bit, transfer):
    result = [None] * len(values)
    for n in range(len(values)):
        if n & bit == 0:
            m = n | bit
            result[n], result[m] = mixed_pair(values[n], values[m], transfer(n), transfer(m))
    return result


def kernel(
    src, leaf, st, tt, out,
    src_v, leaf_v, s0, sb, sk, sp, t01, t23, c0, c0p, c1, cb, yk, ys, yp, wm, mb, rb,
    load_sem, own_sem, s_send, s_recv, s3_send, s3_recv, t01_send, t01_recv, t23_send, t23_recv,
    p_send, p_recv, y_send, y_recv, z_send, z_recv, m_send, m_recv, r_send, r_recv,
):
    x = lax.axis_index("gx")
    g = lax.axis_index("gy")
    z = g // 8
    z1 = z // 2
    z0 = z % 2
    a = (z0 + z1) % 2
    other = 1 - a
    yc = g % 8
    core = g % 2
    mate = z + 1 - 2 * z0

    def z_of(a_bit, k):
        return 2 * k + (a_bit + k) % 2

    def remote(source, target, send, recv, device):
        return pltpu.make_async_remote_copy(
            src_ref=source,
            dst_ref=target,
            send_sem=send,
            recv_sem=recv,
            device_id=device,
            device_id_type=MESH,
        )

    def s_copy(level, r):
        to = (yc + r) % 8
        return remote(
            st.at[level + 1, :, :, to],
            sb.at[level, yc],
            s_send.at[level, r],
            s_recv.at[level, r],
            (x, z * 8 + to),
        )

    def s3_copy(far, k, r):
        to = (yc + r) % 8
        return remote(
            st.at[3, :, z_of(other if far else a, k), to],
            (sp if far else sk).at[yc, k],
            s3_send.at[far, k, r],
            s3_recv.at[far, k, r],
            (x, (mate if far else z) * 8 + to),
        )

    def t01_copy(level, i, h):
        to_x = (x + i) % 4
        to_z1 = (z1 + h) % 2
        return remote(
            tt.at[level, to_x, to_z1],
            t01.at[level, x, z1],
            t01_send.at[level, i, h],
            t01_recv.at[level, i, h],
            (to_x, z_of(a, to_z1) * 8 + yc),
        )

    def t23_copy(level, j):
        to_z = (z + j) % 4
        return remote(
            tt.at[level + 2, :, to_z // 2, to_z % 2],
            t23.at[level, z],
            t23_send.at[level, j],
            t23_recv.at[level, j],
            (x, to_z * 8 + yc),
        )

    def p_copy(q):
        return remote(
            c0.at[q], c0p.at[q], p_send.at[q], p_recv.at[q], (x, g + 1 - 2 * core)
        )

    def y_copy(q, r):
        to = (yc + r) % 8
        return remote(
            c1.at[to, q], cb.at[yc, q], y_send.at[q, r], y_recv.at[q, r], (x, z * 8 + to)
        )

    def z_copy(q):
        chunk = pl.ds(2 * q, 2)
        return remote(
            ys.at[chunk], yp.at[chunk], z_send.at[q], z_recv.at[q], (x, mate * 8 + yc)
        )

    def m_copy(q, i, h):
        chunk = pl.ds(2 * q, 2)
        to_x = (x + i) % 4
        to_z0 = (z0 + h) % 2
        return remote(
            wm.at[to_z0, to_x, chunk],
            mb.at[x, a, chunk],
            m_send.at[q, i, h],
            m_recv.at[q, i, h],
            (to_x, (2 * z1 + to_z0) * 8 + yc),
        )

    def r_copy(q, j):
        chunk = pl.ds(2 * q, 2)
        to_z = (z + j) % 4
        return remote(
            rb.at[to_z, :, chunk],
            out.at[:, z, chunk],
            r_send.at[q, j],
            r_recv.at[q, j],
            (x, to_z * 8 + yc),
        )

    near = [(i, h) for h in range(2) for i in (1, 3, 2, 0) if (i, h) != (0, 0)]
    along_y = [2, 6, 4, 1, 3, 7, 5]
    along_z = [1, 3, 2]
    s3_all = [(far, k, r) for r in [0] + along_y for far in (0, 1) for k in (0, 1)]
    s3_sent = [(far, k, r) for far, k, r in s3_all if (far, r) != (0, 0)]

    loads = [
        pltpu.make_async_copy(src, src_v, load_sem.at[0]),
        pltpu.make_async_copy(leaf, leaf_v, load_sem.at[1]),
        pltpu.make_async_copy(st.at[0], s0, load_sem.at[2]),
    ]
    for copy in loads:
        copy.start()
    own_s = [
        pltpu.make_async_copy(st.at[n + 1, :, :, yc], sb.at[n, yc], own_sem.at[n])
        for n in range(2)
    ]
    own_s3 = [
        pltpu.make_async_copy(st.at[3, :, z_of(a, k), yc], sk.at[yc, k], own_sem.at[2 + k])
        for k in range(2)
    ]
    own_t = [
        pltpu.make_async_copy(tt.at[n, x, z1], t01.at[n, x, z1], own_sem.at[4 + n])
        for n in range(2)
    ] + [
        pltpu.make_async_copy(tt.at[n + 2, :, z1, z0], t23.at[n, z], own_sem.at[6 + n])
        for n in range(2)
    ]
    for copy in own_s + own_s3 + own_t:
        copy.start()

    barrier = pltpu.get_barrier_semaphore()
    peers = [(x, z * 8 + (yc + r) % 8) for r in range(1, 8)]
    peers += [(x, mate * 8 + (yc + r) % 8) for r in range(8)]
    peers += [(x, ((z + 2) % 4) * 8 + yc), (x, ((mate + 2) % 4) * 8 + yc)]
    for i in range(1, 4):
        for to_z in (z, mate, z_of(a, 1 - z1)):
            peers.append(((x + i) % 4, to_z * 8 + yc))
    for peer in peers:
        pl.semaphore_signal(barrier, inc=1, device_id=peer, device_id_type=MESH)

    loads[0].wait()
    loads[1].wait()

    def leaf_body(n, carry):
        for i in range(8):
            v = src_v[n // 4, n % 4, i]
            c0[n // 4, n % 4, i] = dot(
                leaf_v[n // 4, n % 4, i], jnp.concatenate([v, turned(v)], axis=0)
            )
        return carry

    lax.fori_loop(0, 16, leaf_body, 0)
    pl.semaphore_wait(barrier, len(peers))

    for q in range(4):
        p_copy(q).start()
    for level in range(2):
        for r in along_y:
            s_copy(level, r).start()
    for level in range(2):
        for i, h in near:
            t01_copy(level, i, h).start()
        for j in along_z:
            t23_copy(level, j).start()

    loads[2].wait()

    def first_body(q, carry):
        p_copy(q).wait_recv()
        for n in range(4):
            for i in range(8):
                c1[i, q, n] = mixed(c0[q, n, i], c0p[q, n, i], s0[q, n, i])
        for r in along_y:
            y_copy(q, r).start()
        return carry

    lax.fori_loop(0, 4, first_body, 0)
    for far, k, r in s3_sent:
        s3_copy(far, k, r).start()
    cb[yc] = c1[yc]

    for level in range(2):
        own_s[level].wait()
        for r in along_y:
            s_copy(level, r).wait_recv()

    def y_body(q, carry):
        for r in along_y:
            y_copy(q, r).wait_recv()
        for k in range(2):
            for target, a_bit in ((ys, other), (yk, a)):
                vz = z_of(a_bit, k)
                values = [cb[i, q, vz] for i in range(8)]
                for level, bit in enumerate((2, 4)):
                    values = paired(values, bit, lambda i: sb[level, i, q, vz])
                for i in range(8):
                    target[i, k, q] = values[i]
        return carry

    lax.fori_loop(0, 4, y_body, 0)
    for q in range(4):
        z_copy(q).start()
    for copy in own_s3 + own_t:
        copy.wait()
    for far, k, r in s3_sent:
        s3_copy(far, k, r).wait_recv()
    for level in range(2):
        for i, h in near:
            t01_copy(level, i, h).wait_recv()

    def x_body(q, carry):
        z_copy(q).wait_recv()
        for b in range(2):
            i = 2 * q + b
            for k in range(2):
                values = [yk[i, k, n] for n in range(4)] + [yp[i, k, n] for n in range(4)]
                values = paired(
                    values, 4, lambda n: sp[i, k, n - 4] if n >= 4 else sk[i, k, n]
                )
                sides = (z0, 1 - z0)
                for level, bit in enumerate((2, 1)):
                    values = paired(
                        values, bit, lambda n: t01[level, n % 4, k, sides[n // 4], i]
                    )
                for n in range(8):
                    wm[sides[n // 4], n % 4, i, k] = values[n]
        for i, h in near:
            m_copy(q, i, h).start()
        chunk = pl.ds(2 * q, 2)
        mb[x, a, chunk] = wm[z0, x, chunk]
        return carry

    lax.fori_loop(0, 4, x_body, 0)
    for level in range(2):
        for j in along_z:
            t23_copy(level, j).wait_recv()

    def last_body(q, carry):
        for i, h in near:
            m_copy(q, i, h).wait_recv()
        for b in range(2):
            i = 2 * q + b
            for n in range(4):
                values = [mb[n, m // 2, i, m % 2] for m in range(4)]
                for level, bit in enumerate((3, 2)):
                    result = [None] * 4
                    for m in range(2):
                        w = m ^ bit
                        result[m], result[w] = mixed_pair(
                            values[m],
                            values[w],
                            t23[level, z_of(m // 2, m % 2), n, i],
                            t23[level, z_of(w // 2, w % 2), n, i],
                        )
                    values = result
                for m in range(4):
                    rb[z_of(m // 2, m % 2), n, i] = values[m]
        for j in along_z:
            r_copy(q, j).start()
        chunk = pl.ds(2 * q, 2)
        out[:, z, chunk] = rb[z, :, chunk]
        return carry

    lax.fori_loop(0, 4, last_body, 0)

    for q in range(4):
        for j in along_z:
            r_copy(q, j).wait()
        for i, h in near:
            m_copy(q, i, h).wait_send()
        p_copy(q).wait_send()
        z_copy(q).wait_send()
        for r in along_y:
            y_copy(q, r).wait_send()
    for level in range(2):
        for r in along_y:
            s_copy(level, r).wait_send()
        for i, h in near:
            t01_copy(level, i, h).wait_send()
        for j in along_z:
            t23_copy(level, j).wait_send()
    for far, k, r in s3_sent:
        s3_copy(far, k, r).wait_send()


def local(source_values, leaf_maps, source_transfers, target_transfers):
    dma = pltpu.SemaphoreType.DMA
    box = (32, 128)

    def vmem(*shape):
        return pltpu.VMEM(shape + box, BF16)

    out = pl.pallas_call(
        kernel,
        out_shape=jax.ShapeDtypeStruct((4, 4, 8) + box, BF16),
        in_specs=[pl.BlockSpec(memory_space=pl.ANY)] * 4,
        out_specs=pl.BlockSpec(memory_space=pltpu.VMEM),
        scratch_shapes=[
            pltpu.VMEM((4, 4, 8, 64, 128), BF16),
            vmem(4, 4, 8),
            vmem(4, 4, 8),
            vmem(2, 8, 4, 4),
            vmem(8, 2, 4),
            vmem(8, 2, 4),
            vmem(2, 4, 2, 2, 8),
            vmem(2, 4, 4, 8),
            vmem(4, 4, 8),
            vmem(4, 4, 8),
            vmem(8, 4, 4),
            vmem(8, 4, 4),
            vmem(8, 2, 4),
            vmem(8, 2, 4),
            vmem(8, 2, 4),
            vmem(2, 4, 8, 2),
            vmem(4, 2, 8, 2),
            vmem(4, 4, 8),
            dma((3,)),
            dma((8,)),
            dma((2, 8)),
            dma((2, 8)),
            dma((2, 2, 8)),
            dma((2, 2, 8)),
            dma((2, 4, 2)),
            dma((2, 4, 2)),
            dma((2, 4)),
            dma((2, 4)),
            dma((4,)),
            dma((4,)),
            dma((4, 8)),
            dma((4, 8)),
            dma((4,)),
            dma((4,)),
            dma((4, 4, 2)),
            dma((4, 4, 2)),
            dma((4, 4)),
            dma((4, 4)),
        ],
        compiler_params=pltpu.CompilerParams(
            collective_id=0, has_side_effects=True, vmem_limit_bytes=67_043_328
        ),
    )(
        source_values.reshape(4, 4, 8, 64, 128),
        leaf_maps.reshape((4, 4, 8) + box),
        source_transfers.reshape((4, 4, 4, 8) + box),
        target_transfers.reshape((4, 4, 2, 2, 8) + box),
    )
    return out.reshape((128,) + box)


def solution(mesh):
    return jax.shard_map(
        local,
        mesh=mesh,
        in_specs=(
            P(("gx", "gy"), None, None),
            P(("gx", "gy"), None, None),
            P(None, ("gx", "gy"), None, None),
            P(None, ("gx", "gy"), None, None),
        ),
        out_specs=P(("gx", "gy"), None, None),
        check_vma=False,
    )
```

```python
import jax
import jax.numpy as jnp
from jax import lax
from jax.experimental import pallas as pl
from jax.experimental.pallas import tpu as pltpu
from jax.sharding import PartitionSpec as P

MESH = pl.DeviceIdType.MESH
BF16 = jnp.bfloat16
F32 = jnp.float32


def turned(x):
    wide = pltpu.roll(x.astype(F32), 64, x.ndim - 1)
    lane = lax.broadcasted_iota(jnp.int32, wide.shape, wide.ndim - 1)
    return jnp.where(lane < 64, -wide, wide).astype(BF16)


def dot(a, b):
    return jnp.dot(a, b, preferred_element_type=F32).astype(BF16)


def mixed(own, partner, transfer):
    operand = jnp.concatenate([own, turned(own), partner, turned(partner)], axis=0)
    return dot(transfer, operand)


def mixed_pair(a, b, transfer_a, transfer_b):
    ta, tb = turned(a), turned(b)
    out_a = dot(transfer_a, jnp.concatenate([a, ta, b, tb], axis=0))
    out_b = dot(transfer_b, jnp.concatenate([b, tb, a, ta], axis=0))
    return out_a, out_b


def paired(values, bit, transfer):
    result = [None] * len(values)
    for n in range(len(values)):
        if n & bit == 0:
            m = n | bit
            result[n], result[m] = mixed_pair(values[n], values[m], transfer(n), transfer(m))
    return result


NH = 4
CH = 8 // NH


def kernel(
    src, leaf, st, tt, out,
    src_v, leaf_v, s0, sb, sk, sp, t01, t23, c0, c0p, c1, cb, yk, ys, yp, wm, mb, rb,
    load_sem, own_sem, s_send, s_recv, s3_send, s3_recv, t01_send, t01_recv, t23_send, t23_recv,
    p_send, p_recv, y_send, y_recv, z_send, z_recv, m_send, m_recv, r_send, r_recv,
):
    x = lax.axis_index("gx")
    g = lax.axis_index("gy")
    z = g // 8
    z1 = z // 2
    z0 = z % 2
    a = (z0 + z1) % 2
    other = 1 - a
    yc = g % 8
    core = g % 2
    mate = z + 1 - 2 * z0

    def z_of(a_bit, k):
        return 2 * k + (a_bit + k) % 2

    def remote(source, target, send, recv, device):
        return pltpu.make_async_remote_copy(
            src_ref=source,
            dst_ref=target,
            send_sem=send,
            recv_sem=recv,
            device_id=device,
            device_id_type=MESH,
        )

    def s_copy(level, k, r):
        to = (yc + r) % 8
        return remote(
            st.at[level + 1, :, k, :, to],
            sb.at[level, yc, k],
            s_send.at[level, k, r],
            s_recv.at[level, k, r],
            (x, z * 8 + to),
        )

    def s3_copy(far, k, r):
        to = (yc + r) % 8
        return remote(
            st.at[3, :, k, ((other if far else a) + k) % 2, to],
            (sp if far else sk).at[yc, k],
            s3_send.at[far, k, r],
            s3_recv.at[far, k, r],
            (x, (mate if far else z) * 8 + to),
        )

    def t01_copy(level, i, h):
        to_x = (x + i) % 4
        to_z1 = (z1 + h) % 2
        return remote(
            tt.at[level, to_x, to_z1],
            t01.at[level, x, z1],
            t01_send.at[level, i, h],
            t01_recv.at[level, i, h],
            (to_x, z_of(a, to_z1) * 8 + yc),
        )

    def t23_copy(level, j):
        to_z = (z + j) % 4
        return remote(
            tt.at[level + 2, :, to_z // 2, to_z % 2],
            t23.at[level, z],
            t23_send.at[level, j],
            t23_recv.at[level, j],
            (x, to_z * 8 + yc),
        )

    def p_copy(k):
        return remote(
            c0.at[k], c0p.at[k], p_send.at[k], p_recv.at[k], (x, g + 1 - 2 * core)
        )

    def y_copy(k, r):
        to = (yc + r) % 8
        return remote(
            c1.at[to, k], cb.at[yc, k], y_send.at[k, r], y_recv.at[k, r], (x, z * 8 + to)
        )

    def z_copy(k, q):
        chunk = pl.ds(CH * q, CH)
        return remote(
            ys.at[k, chunk], yp.at[k, chunk], z_send.at[k, q], z_recv.at[k, q], (x, mate * 8 + yc)
        )

    def m_copy(k, q, i, h):
        chunk = pl.ds(CH * q, CH)
        to_x = (x + i) % 4
        to_z0 = (z0 + h) % 2
        return remote(
            wm.at[to_z0, to_x, k, chunk],
            mb.at[x, a, k, chunk],
            m_send.at[k, q, i, h],
            m_recv.at[k, q, i, h],
            (to_x, (2 * z1 + to_z0) * 8 + yc),
        )

    def r_copy(q, j):
        chunk = pl.ds(CH * q, CH)
        to_z = (z + j) % 4
        return remote(
            rb.at[to_z, :, chunk],
            out.at[:, z, chunk],
            r_send.at[q, j],
            r_recv.at[q, j],
            (x, to_z * 8 + yc),
        )

    near = [(i, h) for h in range(2) for i in (1, 3, 2, 0) if (i, h) != (0, 0)]
    along_y = [2, 6, 4, 1, 3, 7, 5]
    along_z = [1, 3, 2]
    s3_sent = [(far, r) for r in [0] + along_y for far in (0, 1) if (far, r) != (0, 0)]

    loads = [
        pltpu.make_async_copy(src, src_v, load_sem.at[0]),
        pltpu.make_async_copy(leaf, leaf_v, load_sem.at[1]),
        pltpu.make_async_copy(st.at[0], s0, load_sem.at[2]),
    ]
    for copy in loads:
        copy.start()
    own_s = [
        pltpu.make_async_copy(st.at[n + 1, :, k, :, yc], sb.at[n, yc, k], own_sem.at[2 * k + n])
        for k in range(2)
        for n in range(2)
    ]
    own_s3 = [
        pltpu.make_async_copy(st.at[3, :, k, (a + k) % 2, yc], sk.at[yc, k], own_sem.at[4 + k])
        for k in range(2)
    ]
    own_t = [
        pltpu.make_async_copy(tt.at[n, x, z1], t01.at[n, x, z1], own_sem.at[6 + n])
        for n in range(2)
    ] + [
        pltpu.make_async_copy(tt.at[n + 2, :, z1, z0], t23.at[n, z], own_sem.at[8 + n])
        for n in range(2)
    ]
    for copy in own_s + own_s3 + own_t:
        copy.start()

    barrier = pltpu.get_barrier_semaphore()
    peers = [(x, z * 8 + (yc + r) % 8) for r in range(1, 8)]
    peers += [(x, mate * 8 + (yc + r) % 8) for r in range(8)]
    peers += [(x, ((z + 2) % 4) * 8 + yc), (x, ((mate + 2) % 4) * 8 + yc)]
    for i in range(1, 4):
        for to_z in (z, mate, z_of(a, 1 - z1)):
            peers.append(((x + i) % 4, to_z * 8 + yc))
    for peer in peers:
        pl.semaphore_signal(barrier, inc=1, device_id=peer, device_id_type=MESH)

    loads[0].wait()
    loads[1].wait()

    def leaf_body(n, carry):
        vx, k, j = n // 4, n // 2 % 2, n % 2
        for i in range(8):
            v = src_v[vx, k, j, i]
            c0[k, vx, j, i] = dot(leaf_v[vx, k, j, i], jnp.concatenate([v, turned(v)], axis=0))
        return carry

    lax.fori_loop(0, 16, leaf_body, 0)
    pl.semaphore_wait(barrier, len(peers))

    for k in range(2):
        p_copy(k).start()
    for level in range(2):
        for r in along_y:
            s_copy(level, 0, r).start()
    for level in range(2):
        for i, h in near:
            t01_copy(level, i, h).start()
    for level in range(2):
        for j in along_z:
            t23_copy(level, j).start()

    loads[2].wait()
    for k in range(2):
        p_copy(k).wait_recv()

        def first_body(vx, carry, k=k):
            for j in range(2):
                for i in range(8):
                    c1[i, k, vx, j] = mixed(c0[k, vx, j, i], c0p[k, vx, j, i], s0[vx, k, j, i])
            return carry

        lax.fori_loop(0, 4, first_body, 0)
        if k == 1:
            for level in range(2):
                for r in along_y:
                    s_copy(level, 1, r).start()
        for r in along_y:
            y_copy(k, r).start()
        for far, r in s3_sent:
            s3_copy(far, k, r).start()
        cb[yc, k] = c1[yc, k]

    for k in range(2):
        for level in range(2):
            own_s[2 * k + level].wait()
            for r in along_y:
                s_copy(level, k, r).wait_recv()
        for r in along_y:
            y_copy(k, r).wait_recv()

        def y_body(vx, carry, k=k):
            for target, a_bit in ((ys, other), (yk, a)):
                j = (a_bit + k) % 2
                values = [cb[i, k, vx, j] for i in range(8)]
                for level, bit in enumerate((2, 4)):
                    values = paired(values, bit, lambda i: sb[level, i, k, vx, j])
                for i in range(8):
                    target[k, i, vx] = values[i]
            return carry

        lax.fori_loop(0, 4, y_body, 0)
        for q in range(NH):
            z_copy(k, q).start()

        own_s3[k].wait()
        for far, r in s3_sent:
            s3_copy(far, k, r).wait_recv()
        if k == 0:
            for copy in own_t:
                copy.wait()
            for level in range(2):
                for i, h in near:
                    t01_copy(level, i, h).wait_recv()

        sides = (z0, 1 - z0)

        def x_body(q, carry, k=k):
            z_copy(k, q).wait_recv()
            for b in range(CH):
                i = CH * q + b
                values = [yk[k, i, n] for n in range(4)] + [yp[k, i, n] for n in range(4)]
                values = paired(
                    values, 4, lambda n: sp[i, k, n - 4] if n >= 4 else sk[i, k, n]
                )
                for level, bit in enumerate((2, 1)):
                    values = paired(
                        values, bit, lambda n: t01[level, n % 4, k, sides[n // 4], i]
                    )
                for n in range(8):
                    wm[sides[n // 4], n % 4, k, i] = values[n]
            for i, h in near:
                m_copy(k, q, i, h).start()
            chunk = pl.ds(CH * q, CH)
            mb[x, a, k, chunk] = wm[z0, x, k, chunk]
            return carry

        lax.fori_loop(0, NH, x_body, 0)

    for level in range(2):
        for j in along_z:
            t23_copy(level, j).wait_recv()

    def last_body(q, carry):
        for k in range(2):
            for i, h in near:
                m_copy(k, q, i, h).wait_recv()
        for b in range(CH):
            i = CH * q + b
            for n in range(4):
                values = [mb[n, m // 2, m % 2, i] for m in range(4)]
                for level, bit in enumerate((3, 2)):
                    result = [None] * 4
                    for m in range(2):
                        w = m ^ bit
                        result[m], result[w] = mixed_pair(
                            values[m],
                            values[w],
                            t23[level, z_of(m // 2, m % 2), n, i],
                            t23[level, z_of(w // 2, w % 2), n, i],
                        )
                    values = result
                for m in range(4):
                    rb[z_of(m // 2, m % 2), n, i] = values[m]
        for j in along_z:
            r_copy(q, j).start()
        chunk = pl.ds(CH * q, CH)
        out[:, z, chunk] = rb[z, :, chunk]
        return carry

    lax.fori_loop(0, NH, last_body, 0)

    for q in range(NH):
        for j in along_z:
            r_copy(q, j).wait()
        for k in range(2):
            z_copy(k, q).wait_send()
            for i, h in near:
                m_copy(k, q, i, h).wait_send()
    for k in range(2):
        p_copy(k).wait_send()
        for r in along_y:
            y_copy(k, r).wait_send()
            for level in range(2):
                s_copy(level, k, r).wait_send()
        for far, r in s3_sent:
            s3_copy(far, k, r).wait_send()
    for level in range(2):
        for i, h in near:
            t01_copy(level, i, h).wait_send()
        for j in along_z:
            t23_copy(level, j).wait_send()


def local(source_values, leaf_maps, source_transfers, target_transfers):
    dma = pltpu.SemaphoreType.DMA
    box = (32, 128)

    def vmem(*shape):
        return pltpu.VMEM(shape + box, BF16)

    out = pl.pallas_call(
        kernel,
        out_shape=jax.ShapeDtypeStruct((4, 4, 8) + box, BF16),
        in_specs=[pl.BlockSpec(memory_space=pl.ANY)] * 4,
        out_specs=pl.BlockSpec(memory_space=pltpu.VMEM),
        scratch_shapes=[
            pltpu.VMEM((4, 2, 2, 8, 64, 128), BF16),
            vmem(4, 2, 2, 8),
            vmem(4, 2, 2, 8),
            vmem(2, 8, 2, 4, 2),
            vmem(8, 2, 4),
            vmem(8, 2, 4),
            vmem(2, 4, 2, 2, 8),
            vmem(2, 4, 4, 8),
            vmem(2, 4, 2, 8),
            vmem(2, 4, 2, 8),
            vmem(8, 2, 4, 2),
            vmem(8, 2, 4, 2),
            vmem(2, 8, 4),
            vmem(2, 8, 4),
            vmem(2, 8, 4),
            vmem(2, 4, 2, 8),
            vmem(4, 2, 2, 8),
            vmem(4, 4, 8),
            dma((3,)),
            dma((10,)),
            dma((2, 2, 8)),
            dma((2, 2, 8)),
            dma((2, 2, 8)),
            dma((2, 2, 8)),
            dma((2, 4, 2)),
            dma((2, 4, 2)),
            dma((2, 4)),
            dma((2, 4)),
            dma((2,)),
            dma((2,)),
            dma((2, 8)),
            dma((2, 8)),
            dma((2, NH)),
            dma((2, NH)),
            dma((2, NH, 4, 2)),
            dma((2, NH, 4, 2)),
            dma((NH, 4)),
            dma((NH, 4)),
        ],
        compiler_params=pltpu.CompilerParams(
            collective_id=0, has_side_effects=True, vmem_limit_bytes=67_043_328
        ),
    )(
        source_values.reshape(4, 2, 2, 8, 64, 128),
        leaf_maps.reshape((4, 2, 2, 8) + box),
        source_transfers.reshape((4, 4, 2, 2, 8) + box),
        target_transfers.reshape((4, 4, 2, 2, 8) + box),
    )
    return out.reshape((128,) + box)


def solution(mesh):
    return jax.shard_map(
        local,
        mesh=mesh,
        in_specs=(
            P(("gx", "gy"), None, None),
            P(("gx", "gy"), None, None),
            P(None, ("gx", "gy"), None, None),
            P(None, ("gx", "gy"), None, None),
        ),
        out_specs=P(("gx", "gy"), None, None),
        check_vma=False,
    )
```

```python
import jax
import jax.numpy as jnp
from jax import lax
from jax.experimental import pallas as pl
from jax.experimental.pallas import tpu as pltpu
from jax.sharding import PartitionSpec as P

MESH = pl.DeviceIdType.MESH
BF16 = jnp.bfloat16
F32 = jnp.float32


def turned(x):
    wide = pltpu.roll(x.astype(F32), 64, x.ndim - 1)
    lane = lax.broadcasted_iota(jnp.int32, wide.shape, wide.ndim - 1)
    return jnp.where(lane < 64, -wide, wide).astype(BF16)


def dot(a, b):
    return jnp.dot(a, b, preferred_element_type=F32).astype(BF16)


def mixed(own, partner, transfer):
    operand = jnp.concatenate([own, turned(own), partner, turned(partner)], axis=0)
    return dot(transfer, operand)


def mixed_pair(a, b, transfer_a, transfer_b):
    ta, tb = turned(a), turned(b)
    out_a = dot(transfer_a, jnp.concatenate([a, ta, b, tb], axis=0))
    out_b = dot(transfer_b, jnp.concatenate([b, tb, a, ta], axis=0))
    return out_a, out_b


def paired(values, bit, transfer):
    result = [None] * len(values)
    for n in range(len(values)):
        if n & bit == 0:
            m = n | bit
            result[n], result[m] = mixed_pair(values[n], values[m], transfer(n), transfer(m))
    return result


NH = 4
CH = 8 // NH


def kernel(
    src, leaf, st, tt, out,
    src_v, leaf_v, s0, sb, sq, t01, t23, c0, c0p, c1, cb, yk, ys, yp, wm, mb, rb,
    load_sem, own_sem, s_recv, s3_recv, t_recv, p_recv, y_recv, z_recv, m_recv, r_recv, sent,
):
    x = lax.axis_index("gx")
    g = lax.axis_index("gy")
    z = g // 8
    z1 = z // 2
    z0 = z % 2
    a = (z0 + z1) % 2
    other = 1 - a
    yc = g % 8
    core = g % 2
    mate = z + 1 - 2 * z0

    def z_of(a_bit, k):
        return 2 * k + (a_bit + k) % 2

    def remote(source, target, send, recv, device):
        return pltpu.make_async_remote_copy(
            src_ref=source,
            dst_ref=target,
            send_sem=sent.at[send],
            recv_sem=recv,
            device_id=device,
            device_id_type=MESH,
        )

    def drain(ref, sem):
        pltpu.make_async_copy(ref, ref, sem).wait()

    def s_copy(k, r):
        to = (yc + r) % 8
        return remote(
            st.at[pl.ds(1, 2), :, k, :, to], sb.at[:, yc, k], 0, s_recv.at[k], (x, z * 8 + to)
        )

    def s3_copy(far, k, r):
        to = (yc + r) % 8
        return remote(
            st.at[3, :, k, ((other if far else a) + k) % 2, to],
            sq.at[8 * far + yc, k],
            1,
            s3_recv.at[k],
            (x, (mate if far else z) * 8 + to),
        )

    def t01_copy(i, h):
        to_x = (x + i) % 4
        to_z1 = (z1 + h) % 2
        return remote(
            tt.at[pl.ds(0, 2), to_x, to_z1],
            t01.at[:, 2 * x + z1],
            2,
            t_recv.at[0],
            (to_x, z_of(a, to_z1) * 8 + yc),
        )

    def t23_copy(level, j):
        to_z = (z + j) % 4
        return remote(
            tt.at[level + 2, :, to_z // 2, to_z % 2],
            t23.at[level, z],
            3,
            t_recv.at[1 + level],
            (x, to_z * 8 + yc),
        )

    def p_copy(k):
        return remote(c0.at[k], c0p.at[k], 4, p_recv.at[k], (x, g + 1 - 2 * core))

    def y_copy(k, r):
        to = (yc + r) % 8
        return remote(c1.at[to, k], cb.at[yc, k], 5, y_recv.at[k], (x, z * 8 + to))

    def z_copy(k, q):
        chunk = pl.ds(CH * q, CH)
        return remote(
            ys.at[k, chunk], yp.at[k, chunk], 6, z_recv.at[k, q], (x, mate * 8 + yc)
        )

    def m_copy(k, q, i, h):
        chunk = pl.ds(CH * q, CH)
        to_x = (x + i) % 4
        to_z0 = (z0 + h) % 2
        return remote(
            wm.at[to_z0, to_x, k, chunk],
            mb.at[2 * x + a, k, chunk],
            7,
            m_recv.at[q],
            (to_x, (2 * z1 + to_z0) * 8 + yc),
        )

    def r_copy(q, j):
        chunk = pl.ds(CH * q, CH)
        to_z = (z + j) % 4
        return remote(
            rb.at[to_z, :, chunk], out.at[:, z, chunk], 8, r_recv, (x, to_z * 8 + yc)
        )

    near = [(i, h) for h in range(2) for i in (1, 3, 2, 0) if (i, h) != (0, 0)]
    along_y = [2, 6, 4, 1, 3, 7, 5]
    along_z = [1, 3, 2]
    s3_sent = [(far, r) for r in [0] + along_y for far in (0, 1) if (far, r) != (0, 0)]

    loads = [
        pltpu.make_async_copy(src, src_v, load_sem.at[0]),
        pltpu.make_async_copy(leaf, leaf_v, load_sem.at[1]),
        pltpu.make_async_copy(st.at[0], s0, load_sem.at[2]),
    ]
    for copy in loads:
        copy.start()
    own_s = [
        pltpu.make_async_copy(st.at[pl.ds(1, 2), :, k, :, yc], sb.at[:, yc, k], own_sem.at[k])
        for k in range(2)
    ]
    own_s3 = [
        pltpu.make_async_copy(st.at[3, :, k, (a + k) % 2, yc], sq.at[yc, k], own_sem.at[2 + k])
        for k in range(2)
    ]
    own_t01 = pltpu.make_async_copy(tt.at[pl.ds(0, 2), x, z1], t01.at[:, 2 * x + z1], own_sem.at[4])
    own_t23 = pltpu.make_async_copy(tt.at[pl.ds(2, 2), :, z1, z0], t23.at[:, z], own_sem.at[5])
    for copy in own_s + own_s3 + [own_t01, own_t23]:
        copy.start()

    barrier = pltpu.get_barrier_semaphore()
    peers = [(x, z * 8 + (yc + r) % 8) for r in range(1, 8)]
    peers += [(x, mate * 8 + (yc + r) % 8) for r in range(8)]
    peers += [(x, ((z + 2) % 4) * 8 + yc), (x, ((mate + 2) % 4) * 8 + yc)]
    for i in range(1, 4):
        for to_z in (z, mate, z_of(a, 1 - z1)):
            peers.append(((x + i) % 4, to_z * 8 + yc))
    for peer in peers:
        pl.semaphore_signal(barrier, inc=1, device_id=peer, device_id_type=MESH)

    loads[0].wait()
    loads[1].wait()

    def leaf_body(n, carry):
        vx, k, j = n // 4, n // 2 % 2, n % 2
        for i in range(8):
            v = src_v[vx, k, j, i]
            c0[k, vx, j, i] = dot(leaf_v[vx, k, j, i], jnp.concatenate([v, turned(v)], axis=0))
        return carry

    lax.fori_loop(0, 16, leaf_body, 0)
    pl.semaphore_wait(barrier, len(peers))

    for k in range(2):
        p_copy(k).start()
    for r in along_y:
        s_copy(0, r).start()
    for i, h in near:
        t01_copy(i, h).start()
    for j in along_z:
        t23_copy(0, j).start()

    loads[2].wait()
    for k in range(2):
        p_copy(k).wait_recv()

        def first_body(vx, carry, k=k):
            for j in range(2):
                for i in range(8):
                    c1[i, k, vx, j] = mixed(c0[k, vx, j, i], c0p[k, vx, j, i], s0[vx, k, j, i])
            return carry

        lax.fori_loop(0, 4, first_body, 0)
        if k == 1:
            for r in along_y:
                s_copy(1, r).start()
        for r in along_y:
            y_copy(k, r).start()
        for far, r in s3_sent:
            s3_copy(far, k, r).start()
        cb[yc, k] = c1[yc, k]

    for k in range(2):
        own_s[k].wait()
        drain(sb.at[:, pl.ds(0, 7), k], s_recv.at[k])
        drain(cb.at[pl.ds(0, 7), k], y_recv.at[k])

        def y_body(vx, carry, k=k):
            for target, a_bit in ((ys, other), (yk, a)):
                j = (a_bit + k) % 2
                values = [cb[i, k, vx, j] for i in range(8)]
                for level, bit in enumerate((2, 4)):
                    values = paired(values, bit, lambda i: sb[level, i, k, vx, j])
                for i in range(8):
                    target[k, i, vx] = values[i]
            return carry

        lax.fori_loop(0, 4, y_body, 0)
        for q in range(NH):
            z_copy(k, q).start()
        if k == 0:
            for j in along_z:
                t23_copy(1, j).start()

        own_s3[k].wait()
        drain(sq.at[pl.ds(0, 15), k], s3_recv.at[k])
        if k == 0:
            own_t01.wait()
            drain(t01.at[:, pl.ds(0, 7)], t_recv.at[0])

        sides = (z0, 1 - z0)

        def x_body(q, carry, k=k):
            z_copy(k, q).wait_recv()
            for b in range(CH):
                i = CH * q + b
                values = [yk[k, i, n] for n in range(4)] + [yp[k, i, n] for n in range(4)]
                values = paired(values, 4, lambda n: sq[8 * (n // 4) + i, k, n % 4])
                for level, bit in enumerate((2, 1)):
                    values = paired(
                        values, bit, lambda n: t01[level, 2 * (n % 4) + k, sides[n // 4], i]
                    )
                for n in range(8):
                    wm[sides[n // 4], n % 4, k, i] = values[n]
            for i, h in near:
                m_copy(k, q, i, h).start()
            chunk = pl.ds(CH * q, CH)
            mb[2 * x + a, k, chunk] = wm[z0, x, k, chunk]
            return carry

        lax.fori_loop(0, NH, x_body, 0)

    own_t23.wait()
    for level in range(2):
        drain(t23.at[level, pl.ds(0, 3)], t_recv.at[1 + level])

    def last_body(q, carry):
        drain(mb.at[pl.ds(0, 7), :, pl.ds(CH * q, CH)], m_recv.at[q])
        for b in range(CH):
            i = CH * q + b
            for n in range(4):
                values = [mb[2 * n + m // 2, m % 2, i] for m in range(4)]
                for level, bit in enumerate((3, 2)):
                    result = [None] * 4
                    for m in range(2):
                        w = m ^ bit
                        result[m], result[w] = mixed_pair(
                            values[m],
                            values[w],
                            t23[level, z_of(m // 2, m % 2), n, i],
                            t23[level, z_of(w // 2, w % 2), n, i],
                        )
                    values = result
                for m in range(4):
                    rb[z_of(m // 2, m % 2), n, i] = values[m]
        for j in along_z:
            r_copy(q, j).start()
        chunk = pl.ds(CH * q, CH)
        out[:, z, chunk] = rb[z, :, chunk]
        return carry

    lax.fori_loop(0, NH, last_body, 0)

    drain(out.at[:, pl.ds(0, 3)], r_recv)
    drain(sb.at[:, pl.ds(0, 7)], sent.at[0])
    drain(sq.at[pl.ds(0, 15)], sent.at[1])
    drain(t01.at[:, pl.ds(0, 7)], sent.at[2])
    drain(t23.at[:, pl.ds(0, 3)], sent.at[3])
    drain(c0, sent.at[4])
    drain(cb.at[pl.ds(0, 7)], sent.at[5])
    drain(ys, sent.at[6])
    drain(mb.at[pl.ds(0, 7)], sent.at[7])
    drain(out.at[:, pl.ds(0, 3)], sent.at[8])


def local(source_values, leaf_maps, source_transfers, target_transfers):
    dma = pltpu.SemaphoreType.DMA
    box = (32, 128)

    def vmem(*shape):
        return pltpu.VMEM(shape + box, BF16)

    out = pl.pallas_call(
        kernel,
        out_shape=jax.ShapeDtypeStruct((4, 4, 8) + box, BF16),
        in_specs=[pl.BlockSpec(memory_space=pl.ANY)] * 4,
        out_specs=pl.BlockSpec(memory_space=pltpu.VMEM),
        scratch_shapes=[
            pltpu.VMEM((4, 2, 2, 8, 64, 128), BF16),
            vmem(4, 2, 2, 8),
            vmem(4, 2, 2, 8),
            vmem(2, 8, 2, 4, 2),
            vmem(16, 2, 4),
            vmem(2, 8, 2, 8),
            vmem(2, 4, 4, 8),
            vmem(2, 4, 2, 8),
            vmem(2, 4, 2, 8),
            vmem(8, 2, 4, 2),
            vmem(8, 2, 4, 2),
            vmem(2, 8, 4),
            vmem(2, 8, 4),
            vmem(2, 8, 4),
            vmem(2, 4, 2, 8),
            vmem(8, 2, 8),
            vmem(4, 4, 8),
            dma((3,)),
            dma((6,)),
            dma((2,)),
            dma((2,)),
            dma((3,)),
            dma((2,)),
            dma((2,)),
            dma((2, NH)),
            dma((NH,)),
            dma,
            dma((9,)),
        ],
        compiler_params=pltpu.CompilerParams(
            collective_id=0, has_side_effects=True, vmem_limit_bytes=54000 * 1024
        ),
    )(
        source_values.reshape(4, 2, 2, 8, 64, 128),
        leaf_maps.reshape((4, 2, 2, 8) + box),
        source_transfers.reshape((4, 4, 2, 2, 8) + box),
        target_transfers.reshape((4, 4, 2, 2, 8) + box),
    )
    return out.reshape((128,) + box)


def solution(mesh):
    return jax.shard_map(
        local,
        mesh=mesh,
        in_specs=(
            P(("gx", "gy"), None, None),
            P(("gx", "gy"), None, None),
            P(None, ("gx", "gy"), None, None),
            P(None, ("gx", "gy"), None, None),
        ),
        out_specs=P(("gx", "gy"), None, None),
        check_vma=False,
    )
```

```python
import jax
import jax.numpy as jnp
from jax import lax
from jax.experimental import pallas as pl
from jax.experimental.pallas import tpu as pltpu
from jax.sharding import PartitionSpec as P

MESH = pl.DeviceIdType.MESH
BF16 = jnp.bfloat16
F32 = jnp.float32


def turned(x):
    lane = lax.broadcasted_iota(jnp.int32, (1, 128), 1)
    return pltpu.roll(x, 64, 1) * jnp.where(lane < 64, -1.0, 1.0).astype(BF16)


def dot(a, b):
    return jnp.dot(a, b, preferred_element_type=F32).astype(BF16)


def mixed(own, partner, transfer):
    operand = jnp.concatenate([own, turned(own), partner, turned(partner)], axis=0)
    return dot(transfer, operand)


def mixed_pair(a, b, transfer_a, transfer_b):
    operand = jnp.concatenate([a, turned(a), b, turned(b)], axis=0)
    out = dot(jnp.concatenate([transfer_a, pltpu.roll(transfer_b, 64, 1)], axis=0), operand)
    return out[:32], out[32:]


def paired(values, bit, transfer):
    result = [None] * len(values)
    for n in range(len(values)):
        if n < n ^ bit:
            m = n ^ bit
            result[n], result[m] = mixed_pair(values[n], values[m], transfer(n), transfer(m))
    return result


NH = 4
CH = 8 // NH
LAG = 2


def kernel(
    src, leaf, st, tt, out,
    src_v, leaf_v, s0, sb, sq, t01, t23, c0, c0p, c1, cb, yk, ys, yp, wm, mb, rb,
    load_sem, own_sem, s_recv, s3_recv, t_recv, p_recv, y_recv, z_recv, m_recv, r_recv, sent,
):
    x = lax.axis_index("gx")
    g = lax.axis_index("gy")
    z = g // 8
    z1 = z // 2
    z0 = z % 2
    a = (z0 + z1) % 2
    other = 1 - a
    yc = g % 8
    core = g % 2
    mate = z + 1 - 2 * z0

    def z_of(a_bit, k):
        return 2 * k + (a_bit + k) % 2

    def remote(source, target, send, recv, device):
        return pltpu.make_async_remote_copy(
            src_ref=source,
            dst_ref=target,
            send_sem=sent.at[send],
            recv_sem=recv,
            device_id=device,
            device_id_type=MESH,
        )

    def drain(ref, sem):
        pltpu.make_async_copy(ref, ref, sem).wait()

    def s_copy(k, r):
        to = (yc + r) % 8
        return remote(
            st.at[pl.ds(1, 2), :, k, :, to], sb.at[:, yc, k], 0, s_recv.at[k], (x, z * 8 + to)
        )

    def s3_copy(far, k, r):
        to = (yc + r) % 8
        return remote(
            st.at[3, :, k, ((other if far else a) + k) % 2, to],
            sq.at[8 * far + yc, k],
            1,
            s3_recv.at[k],
            (x, (mate if far else z) * 8 + to),
        )

    def t01_copy(i, h):
        to_x = (x + i) % 4
        to_z1 = (z1 + h) % 2
        return remote(
            tt.at[pl.ds(0, 2), to_x, to_z1],
            t01.at[:, 2 * x + z1],
            2,
            t_recv.at[0],
            (to_x, z_of(a, to_z1) * 8 + yc),
        )

    def t23_copy(level, to_z):
        return remote(
            tt.at[level + 2, :, to_z // 2, to_z % 2],
            t23.at[level, z],
            3,
            t_recv.at[1 + level],
            (x, to_z * 8 + yc),
        )

    def p_copy(k):
        return remote(c0.at[k], c0p.at[k], 4, p_recv.at[k], (x, g + 1 - 2 * core))

    def y_copy(k, r):
        to = (yc + r) % 8
        return remote(c1.at[to, k], cb.at[yc, k], 5, y_recv.at[k], (x, z * 8 + to))

    def z_copy(k, q):
        chunk = pl.ds(CH * q, CH)
        return remote(
            ys.at[k, chunk], yp.at[k, chunk], 6, z_recv.at[k, q], (x, mate * 8 + yc)
        )

    def m_copy(k, q, i, h):
        chunk = pl.ds(CH * q, CH)
        to_x = (x + i) % 4
        to_z0 = (z0 + h) % 2
        return remote(
            wm.at[to_z0, to_x, k, chunk],
            mb.at[2 * x + a, k, chunk],
            7,
            m_recv.at[q],
            (to_x, (2 * z1 + to_z0) * 8 + yc),
        )

    def r_copy(q, j):
        chunk = pl.ds(CH * q, CH)
        to_z = (z + j) % 4
        return remote(
            rb.at[to_z, :, chunk], out.at[:, z, chunk], 8, r_recv, (x, to_z * 8 + yc)
        )

    near = [(i, h) for h in range(2) for i in (1, 3, 2, 0) if (i, h) != (0, 0)]
    along_y = [2, 6, 4, 1, 3, 7, 5]
    along_z = [1, 3, 2]
    s3_sent = [(far, r) for r in [0] + along_y for far in (0, 1) if (far, r) != (0, 0)]

    loads = [
        pltpu.make_async_copy(src, src_v, load_sem.at[0]),
        pltpu.make_async_copy(leaf, leaf_v, load_sem.at[1]),
        pltpu.make_async_copy(st.at[0], s0, load_sem.at[2]),
    ]
    for copy in loads:
        copy.start()
    own_s = [
        pltpu.make_async_copy(st.at[pl.ds(1, 2), :, k, :, yc], sb.at[:, yc, k], own_sem.at[k])
        for k in range(2)
    ]
    own_s3 = [
        pltpu.make_async_copy(st.at[3, :, k, (a + k) % 2, yc], sq.at[yc, k], own_sem.at[2 + k])
        for k in range(2)
    ]
    own_t01 = pltpu.make_async_copy(tt.at[pl.ds(0, 2), x, z1], t01.at[:, 2 * x + z1], own_sem.at[4])
    own_t23 = pltpu.make_async_copy(tt.at[pl.ds(2, 2), :, z1, z0], t23.at[:, z], own_sem.at[5])
    for copy in own_s + own_s3 + [own_t01, own_t23]:
        copy.start()

    barrier = pltpu.get_barrier_semaphore()
    peers = [(x, z * 8 + (yc + r) % 8) for r in range(1, 8)]
    peers += [(x, mate * 8 + (yc + r) % 8) for r in range(8)]
    peers += [(x, ((z + 2) % 4) * 8 + yc), (x, ((mate + 2) % 4) * 8 + yc)]
    for i in range(1, 4):
        for to_z in (z, mate, z_of(a, 1 - z1)):
            peers.append(((x + i) % 4, to_z * 8 + yc))
    for peer in peers:
        pl.semaphore_signal(barrier, inc=1, device_id=peer, device_id_type=MESH)

    pl.semaphore_wait(barrier, len(peers))
    for r in along_y:
        s_copy(0, r).start()
    for i, h in near:
        t01_copy(i, h).start()
    for to_z in (mate, (z + 2) % 4, (mate + 2) % 4):
        t23_copy(0, to_z).start()

    loads[0].wait()
    loads[1].wait()
    for k in range(2):

        def leaf_body(n, carry, k=k):
            for w in range(4):
                vx, j = 2 * n + w // 2, w % 2
                for i in range(8):
                    v = src_v[vx, k, j, i]
                    c0[k, vx, j, i] = dot(
                        leaf_v[vx, k, j, i], jnp.concatenate([v, turned(v)], axis=0)
                    )
            return carry

        lax.fori_loop(0, 2, leaf_body, 0)
        p_copy(k).start()

    loads[2].wait()
    for k in range(2):
        p_copy(k).wait_recv()

        def first_body(n, carry, k=k):
            for w in range(4):
                vx, j = 2 * n + w // 2, w % 2
                for i in range(8):
                    c1[i, k, vx, j] = mixed(c0[k, vx, j, i], c0p[k, vx, j, i], s0[vx, k, j, i])
            return carry

        lax.fori_loop(0, 2, first_body, 0)
        for r in along_y:
            y_copy(k, r).start()
        if k == 0:
            for far, r in s3_sent:
                s3_copy(far, 0, r).start()
            for to_z in (mate, (z + 2) % 4, (mate + 2) % 4):
                t23_copy(1, to_z).start()
            for r in along_y:
                s_copy(1, r).start()
        cb[yc, k] = c1[yc, k]

    sides = (z0, 1 - z0)

    def x_stage(k, q):
        z_copy(k, q).wait_recv()

        rows = [CH * q + b for b in range(CH)]
        values = [v for i in rows for m in (yk, yp) for v in [m[k, i, n] for n in range(4)]]
        values = paired(
            values, 4, lambda n: sq[8 * (n // 4 % 2) + rows[n // 8], k, n % 4]
        )
        for level, bit in enumerate((2, 1)):
            values = paired(
                values,
                bit,
                lambda n: t01[level, 2 * (n % 4) + k, sides[n // 4 % 2], rows[n // 8]],
            )
        for n in range(8 * CH):
            wm[sides[n // 4 % 2], n % 4, k, rows[n // 8]] = values[n]
        for i, h in near:
            m_copy(k, q, i, h).start()
        chunk = pl.ds(CH * q, CH)
        mb[2 * x + a, k, chunk] = wm[z0, x, k, chunk]

    def last_stage(q):
        drain(mb.at[pl.ds(0, 7), :, pl.ds(CH * q, CH)], m_recv.at[q])

        places = [(CH * q + b, n) for b in range(CH) for n in range(4)]
        values = [mb[2 * n + m // 2, m % 2, i] for i, n in places for m in range(4)]
        for level, bit in enumerate((3, 2)):
            values = paired(
                values,
                bit,
                lambda w: t23[
                    level, z_of(w % 4 // 2, w % 2), places[w // 4][1], places[w // 4][0]
                ],
            )
        for w in range(len(values)):
            rb[z_of(w % 4 // 2, w % 2), places[w // 4][1], places[w // 4][0]] = values[w]
        for j in along_z:
            r_copy(q, j).start()
        chunk = pl.ds(CH * q, CH)
        out[:, z, chunk] = rb[z, :, chunk]

    for k in range(2):
        own_s[k].wait()
        drain(sb.at[:, pl.ds(0, 7), k], s_recv.at[k])
        drain(cb.at[pl.ds(0, 7), k], y_recv.at[k])

        def y_body(h, carry, k=k):
            columns = [
                (2 * h + n, target, (a_bit + k) % 2)
                for n in range(2)
                for target, a_bit in ((ys, other), (yk, a))
            ]
            values = [cb[i, k, vx, j] for vx, _, j in columns for i in range(8)]
            for level, bit in enumerate((2, 4)):
                values = paired(
                    values,
                    bit,
                    lambda n: sb[level, n % 8, k, columns[n // 8][0], columns[n // 8][2]],
                )
            for n in range(32):
                vx, target, _ = columns[n // 8]
                target[k, n % 8, vx] = values[n]
            return carry

        lax.fori_loop(0, 2, y_body, 0)
        for q in range(NH):
            z_copy(k, q).start()
        if k == 0:
            for far, r in s3_sent:
                s3_copy(far, 1, r).start()

        own_s3[k].wait()
        drain(sq.at[pl.ds(0, 15), k], s3_recv.at[k])
        if k == 0:
            own_t01.wait()
            drain(t01.at[:, pl.ds(0, 7)], t_recv.at[0])
            for q in range(NH):
                x_stage(0, q)

    own_t23.wait()
    for q in range(NH + LAG):
        if q < NH:
            x_stage(1, q)
        if q == LAG:
            for level in range(2):
                drain(t23.at[level, pl.ds(0, 3)], t_recv.at[1 + level])
        if q >= LAG:
            last_stage(q - LAG)

    drain(out.at[:, pl.ds(0, 3)], r_recv)
    drain(sb.at[:, pl.ds(0, 7)], sent.at[0])
    drain(sq.at[pl.ds(0, 15)], sent.at[1])
    drain(t01.at[:, pl.ds(0, 7)], sent.at[2])
    drain(t23.at[:, pl.ds(0, 3)], sent.at[3])
    drain(c0, sent.at[4])
    drain(cb.at[pl.ds(0, 7)], sent.at[5])
    drain(ys, sent.at[6])
    drain(mb.at[pl.ds(0, 7)], sent.at[7])
    drain(out.at[:, pl.ds(0, 3)], sent.at[8])


def local(source_values, leaf_maps, source_transfers, target_transfers):
    dma = pltpu.SemaphoreType.DMA
    box = (32, 128)

    def vmem(*shape):
        return pltpu.VMEM(shape + box, BF16)

    out = pl.pallas_call(
        kernel,
        out_shape=jax.ShapeDtypeStruct((4, 4, 8) + box, BF16),
        in_specs=[pl.BlockSpec(memory_space=pl.ANY)] * 4,
        out_specs=pl.BlockSpec(memory_space=pltpu.VMEM),
        scratch_shapes=[
            pltpu.VMEM((4, 2, 2, 8, 64, 128), BF16),
            vmem(4, 2, 2, 8),
            vmem(4, 2, 2, 8),
            vmem(2, 8, 2, 4, 2),
            vmem(16, 2, 4),
            vmem(2, 8, 2, 8),
            vmem(2, 4, 4, 8),
            vmem(2, 4, 2, 8),
            vmem(2, 4, 2, 8),
            vmem(8, 2, 4, 2),
            vmem(8, 2, 4, 2),
            vmem(2, 8, 4),
            vmem(2, 8, 4),
            vmem(2, 8, 4),
            vmem(2, 4, 2, 8),
            vmem(8, 2, 8),
            vmem(4, 4, 8),
            dma((3,)),
            dma((6,)),
            dma((2,)),
            dma((2,)),
            dma((3,)),
            dma((2,)),
            dma((2,)),
            dma((2, NH)),
            dma((NH,)),
            dma,
            dma((9,)),
        ],
        compiler_params=pltpu.CompilerParams(
            collective_id=0, has_side_effects=True, vmem_limit_bytes=54000 * 1024
        ),
    )(
        source_values.reshape(4, 2, 2, 8, 64, 128),
        leaf_maps.reshape((4, 2, 2, 8) + box),
        source_transfers.reshape((4, 4, 2, 2, 8) + box),
        target_transfers.reshape((4, 4, 2, 2, 8) + box),
    )
    return out.reshape((128,) + box)


def solution(mesh):
    return jax.shard_map(
        local,
        mesh=mesh,
        in_specs=(
            P(("gx", "gy"), None, None),
            P(("gx", "gy"), None, None),
            P(None, ("gx", "gy"), None, None),
            P(None, ("gx", "gy"), None, None),
        ),
        out_specs=P(("gx", "gy"), None, None),
        check_vma=False,
    )
```

```python
import jax
import jax.numpy as jnp
from jax import lax
from jax.experimental import pallas as pl
from jax.experimental.pallas import tpu as pltpu
from jax.sharding import PartitionSpec as P

MESH = pl.DeviceIdType.MESH
BF16 = jnp.bfloat16
F32 = jnp.float32


def turned(x):
    lane = lax.broadcasted_iota(jnp.int32, (1, 128), 1)
    return pltpu.roll(x, 64, 1) * jnp.where(lane < 64, -1.0, 1.0).astype(BF16)


def dot(a, b):
    return jnp.dot(a, b, preferred_element_type=F32).astype(BF16)


def mixed(own, partner, transfer):
    operand = jnp.concatenate([own, turned(own), partner, turned(partner)], axis=0)
    return dot(transfer, operand)


def mixed_pair(a, b, transfer_a, transfer_b):
    operand = jnp.concatenate([a, turned(a), b, turned(b)], axis=0)
    out = dot(jnp.concatenate([transfer_a, pltpu.roll(transfer_b, 64, 1)], axis=0), operand)
    return out[:32], out[32:]


def paired(values, bit, transfer):
    result = [None] * len(values)
    for n in range(len(values)):
        if n < n ^ bit:
            m = n ^ bit
            result[n], result[m] = mixed_pair(values[n], values[m], transfer(n), transfer(m))
    return result


NH = 4
CH = 8 // NH
LAG = 2


def kernel(
    src, leaf, st, tt, out,
    src_v, leaf_v, s0, sb, sq, z3, t01, t23, c0, c0p, c1, cb, yk, ys, yp, wm, mb, rb,
    load_sem, own_sem, s_recv, s3_recv, z3_recv, t_recv, p_recv, y_recv, z_recv, m_recv, r_recv, sent,
):
    x = lax.axis_index("gx")
    g = lax.axis_index("gy")
    z = g // 8
    z1 = z // 2
    z0 = z % 2
    a = (z0 + z1) % 2
    other = 1 - a
    yc = g % 8
    core = g % 2
    mate = z + 1 - 2 * z0

    def z_of(a_bit, k):
        return 2 * k + (a_bit + k) % 2

    def remote(source, target, send, recv, device):
        return pltpu.make_async_remote_copy(
            src_ref=source,
            dst_ref=target,
            send_sem=sent.at[send],
            recv_sem=recv,
            device_id=device,
            device_id_type=MESH,
        )

    def drain(ref, sem):
        pltpu.make_async_copy(ref, ref, sem).wait()

    def s_copy(k, r):
        to = (yc + r) % 8
        return remote(
            st.at[pl.ds(1, 2), :, k, :, to], sb.at[:, yc, k], 0, s_recv.at[k], (x, z * 8 + to)
        )

    def s3_copy(k, r):
        to = (yc + r) % 8
        return remote(
            st.at[3, :, k, (a + k) % 2, to], sq.at[yc, k], 1, s3_recv.at[k], (x, z * 8 + to)
        )

    def cross_copy(k):
        return remote(
            st.at[3, :, k, (other + k) % 2], z3.at[k], 9, z3_recv.at[k], (x, mate * 8 + yc)
        )

    def pass_copy(k, r):
        to = (yc + r) % 8
        return remote(
            z3.at[k, :, to], sq.at[8 + yc, k], 1, s3_recv.at[k], (x, z * 8 + to)
        )

    def t01_copy(i, h):
        to_x = (x + i) % 4
        to_z1 = (z1 + h) % 2
        return remote(
            tt.at[pl.ds(0, 2), to_x, to_z1],
            t01.at[:, 2 * x + z1],
            2,
            t_recv.at[0],
            (to_x, z_of(a, to_z1) * 8 + yc),
        )

    def t23_copy(level, to_z):
        return remote(
            tt.at[level + 2, :, to_z // 2, to_z % 2],
            t23.at[level, z],
            3,
            t_recv.at[1 + level],
            (x, to_z * 8 + yc),
        )

    def p_copy(k):
        return remote(c0.at[k], c0p.at[k], 4, p_recv.at[k], (x, g + 1 - 2 * core))

    def y_copy(k, r):
        to = (yc + r) % 8
        return remote(c1.at[to, k], cb.at[yc, k], 5, y_recv.at[k], (x, z * 8 + to))

    def z_copy(k, q):
        chunk = pl.ds(CH * q, CH)
        return remote(
            ys.at[k, chunk], yp.at[k, chunk], 6, z_recv.at[k, q], (x, mate * 8 + yc)
        )

    def m_copy(k, q, i, h):
        chunk = pl.ds(CH * q, CH)
        to_x = (x + i) % 4
        to_z0 = (z0 + h) % 2
        return remote(
            wm.at[to_z0, to_x, k, chunk],
            mb.at[2 * x + a, k, chunk],
            7,
            m_recv.at[q],
            (to_x, (2 * z1 + to_z0) * 8 + yc),
        )

    def r_copy(q, j):
        chunk = pl.ds(CH * q, CH)
        to_z = (z + j) % 4
        return remote(
            rb.at[to_z, :, chunk], out.at[:, z, chunk], 8, r_recv, (x, to_z * 8 + yc)
        )

    near = [(i, h) for h in range(2) for i in (1, 3, 2, 0) if (i, h) != (0, 0)]
    along_y = [2, 6, 4, 1, 3, 7, 5]
    along_z = [1, 3, 2]

    loads = [
        pltpu.make_async_copy(src, src_v, load_sem.at[0]),
        pltpu.make_async_copy(leaf, leaf_v, load_sem.at[1]),
        pltpu.make_async_copy(st.at[0], s0, load_sem.at[2]),
    ]
    for copy in loads:
        copy.start()
    own_s = [
        pltpu.make_async_copy(st.at[pl.ds(1, 2), :, k, :, yc], sb.at[:, yc, k], own_sem.at[k])
        for k in range(2)
    ]
    own_s3 = [
        pltpu.make_async_copy(st.at[3, :, k, (a + k) % 2, yc], sq.at[yc, k], own_sem.at[2 + k])
        for k in range(2)
    ]
    own_t01 = pltpu.make_async_copy(tt.at[pl.ds(0, 2), x, z1], t01.at[:, 2 * x + z1], own_sem.at[4])
    own_t23 = pltpu.make_async_copy(tt.at[pl.ds(2, 2), :, z1, z0], t23.at[:, z], own_sem.at[5])
    for copy in own_s + own_s3 + [own_t01, own_t23]:
        copy.start()

    barrier = pltpu.get_barrier_semaphore()
    peers = [(x, z * 8 + (yc + r) % 8) for r in range(1, 8)]
    peers += [(x, ((z + j) % 4) * 8 + yc) for j in range(1, 4)]
    for i in range(1, 4):
        for to_z in (z, mate, z_of(a, 1 - z1)):
            peers.append(((x + i) % 4, to_z * 8 + yc))
    for peer in peers:
        pl.semaphore_signal(barrier, inc=1, device_id=peer, device_id_type=MESH)

    pl.semaphore_wait(barrier, len(peers))
    for r in along_y:
        s_copy(0, r).start()
    for k in range(2):
        cross_copy(k).start()
    for i, h in near:
        t01_copy(i, h).start()
    for level in range(2):
        t23_copy(level, mate).start()

    loads[0].wait()
    loads[1].wait()
    for k in range(2):

        def leaf_body(n, carry, k=k):
            for w in range(4):
                vx, j = 2 * n + w // 2, w % 2
                for i in range(8):
                    v = src_v[vx, k, j, i]
                    c0[k, vx, j, i] = dot(
                        leaf_v[vx, k, j, i], jnp.concatenate([v, turned(v)], axis=0)
                    )
            return carry

        lax.fori_loop(0, 2, leaf_body, 0)
        p_copy(k).start()

    def last_source(k):
        for r in along_y:
            s3_copy(k, r).start()
        drain(z3.at[k], z3_recv.at[k])
        for r in along_y:
            pass_copy(k, r).start()
        sq[8 + yc, k] = z3[k, :, yc]

    loads[2].wait()
    for k in range(2):
        p_copy(k).wait_recv()

        def first_body(n, carry, k=k):
            for w in range(4):
                vx, j = 2 * n + w // 2, w % 2
                for i in range(8):
                    c1[i, k, vx, j] = mixed(c0[k, vx, j, i], c0p[k, vx, j, i], s0[vx, k, j, i])
            return carry

        lax.fori_loop(0, 2, first_body, 0)
        for r in along_y:
            y_copy(k, r).start()
        if k == 0:
            last_source(0)
            for r in along_y:
                s_copy(1, r).start()
        cb[yc, k] = c1[yc, k]

    sides = (z0, 1 - z0)

    def x_stage(k, q):
        z_copy(k, q).wait_recv()

        rows = [CH * q + b for b in range(CH)]
        values = [v for i in rows for m in (yk, yp) for v in [m[k, i, n] for n in range(4)]]
        values = paired(
            values, 4, lambda n: sq[8 * (n // 4 % 2) + rows[n // 8], k, n % 4]
        )
        for level, bit in enumerate((2, 1)):
            values = paired(
                values,
                bit,
                lambda n: t01[level, 2 * (n % 4) + k, sides[n // 4 % 2], rows[n // 8]],
            )
        for n in range(8 * CH):
            wm[sides[n // 4 % 2], n % 4, k, rows[n // 8]] = values[n]
        for i, h in near:
            m_copy(k, q, i, h).start()
        chunk = pl.ds(CH * q, CH)
        mb[2 * x + a, k, chunk] = wm[z0, x, k, chunk]

    def last_stage(q):
        drain(mb.at[pl.ds(0, 7), :, pl.ds(CH * q, CH)], m_recv.at[q])

        places = [(CH * q + b, n) for b in range(CH) for n in range(4)]
        values = [mb[2 * n + m // 2, m % 2, i] for i, n in places for m in range(4)]
        for level, bit in enumerate((3, 2)):
            values = paired(
                values,
                bit,
                lambda w: t23[
                    level, z_of(w % 4 // 2, w % 2), places[w // 4][1], places[w // 4][0]
                ],
            )
        for w in range(len(values)):
            rb[z_of(w % 4 // 2, w % 2), places[w // 4][1], places[w // 4][0]] = values[w]
        for j in along_z:
            r_copy(q, j).start()
        chunk = pl.ds(CH * q, CH)
        out[:, z, chunk] = rb[z, :, chunk]

    for k in range(2):
        own_s[k].wait()
        drain(sb.at[:, pl.ds(0, 7), k], s_recv.at[k])
        drain(cb.at[pl.ds(0, 7), k], y_recv.at[k])

        def y_body(h, carry, k=k):
            columns = [
                (2 * h + n, target, (a_bit + k) % 2)
                for n in range(2)
                for target, a_bit in ((ys, other), (yk, a))
            ]
            values = [cb[i, k, vx, j] for vx, _, j in columns for i in range(8)]
            for level, bit in enumerate((2, 4)):
                values = paired(
                    values,
                    bit,
                    lambda n: sb[level, n % 8, k, columns[n // 8][0], columns[n // 8][2]],
                )
            for n in range(32):
                vx, target, _ = columns[n // 8]
                target[k, n % 8, vx] = values[n]
            return carry

        lax.fori_loop(0, 2, y_body, 0)
        for q in range(NH):
            z_copy(k, q).start()
        if k == 0:
            for to_z in ((z + 2) % 4, (mate + 2) % 4):
                for level in range(2):
                    t23_copy(level, to_z).start()
            last_source(1)

        own_s3[k].wait()
        drain(sq.at[pl.ds(0, 14), k], s3_recv.at[k])
        if k == 0:
            own_t01.wait()
            drain(t01.at[:, pl.ds(0, 7)], t_recv.at[0])
            for q in range(NH):
                x_stage(0, q)

    own_t23.wait()
    for q in range(NH + LAG):
        if q < NH:
            x_stage(1, q)
        if q == LAG:
            for level in range(2):
                drain(t23.at[level, pl.ds(0, 3)], t_recv.at[1 + level])
        if q >= LAG:
            last_stage(q - LAG)

    drain(out.at[:, pl.ds(0, 3)], r_recv)
    drain(sb.at[:, pl.ds(0, 7)], sent.at[0])
    drain(sq.at[pl.ds(0, 14)], sent.at[1])
    drain(z3, sent.at[9])
    drain(t01.at[:, pl.ds(0, 7)], sent.at[2])
    drain(t23.at[:, pl.ds(0, 3)], sent.at[3])
    drain(c0, sent.at[4])
    drain(cb.at[pl.ds(0, 7)], sent.at[5])
    drain(ys, sent.at[6])
    drain(mb.at[pl.ds(0, 7)], sent.at[7])
    drain(out.at[:, pl.ds(0, 3)], sent.at[8])


def local(source_values, leaf_maps, source_transfers, target_transfers):
    dma = pltpu.SemaphoreType.DMA
    box = (32, 128)

    def vmem(*shape):
        return pltpu.VMEM(shape + box, BF16)

    out = pl.pallas_call(
        kernel,
        out_shape=jax.ShapeDtypeStruct((4, 4, 8) + box, BF16),
        in_specs=[pl.BlockSpec(memory_space=pl.ANY)] * 4,
        out_specs=pl.BlockSpec(memory_space=pltpu.VMEM),
        scratch_shapes=[
            pltpu.VMEM((4, 2, 2, 8, 64, 128), BF16),
            vmem(4, 2, 2, 8),
            vmem(4, 2, 2, 8),
            vmem(2, 8, 2, 4, 2),
            vmem(16, 2, 4),
            vmem(2, 4, 8),
            vmem(2, 8, 2, 8),
            vmem(2, 4, 4, 8),
            vmem(2, 4, 2, 8),
            vmem(2, 4, 2, 8),
            vmem(8, 2, 4, 2),
            vmem(8, 2, 4, 2),
            vmem(2, 8, 4),
            vmem(2, 8, 4),
            vmem(2, 8, 4),
            vmem(2, 4, 2, 8),
            vmem(8, 2, 8),
            vmem(4, 4, 8),
            dma((3,)),
            dma((6,)),
            dma((2,)),
            dma((2,)),
            dma((2,)),
            dma((3,)),
            dma((2,)),
            dma((2,)),
            dma((2, NH)),
            dma((NH,)),
            dma,
            dma((10,)),
        ],
        compiler_params=pltpu.CompilerParams(
            collective_id=0, has_side_effects=True, vmem_limit_bytes=54000 * 1024
        ),
    )(
        source_values.reshape(4, 2, 2, 8, 64, 128),
        leaf_maps.reshape((4, 2, 2, 8) + box),
        source_transfers.reshape((4, 4, 2, 2, 8) + box),
        target_transfers.reshape((4, 4, 2, 2, 8) + box),
    )
    return out.reshape((128,) + box)


def solution(mesh):
    return jax.shard_map(
        local,
        mesh=mesh,
        in_specs=(
            P(("gx", "gy"), None, None),
            P(("gx", "gy"), None, None),
            P(None, ("gx", "gy"), None, None),
            P(None, ("gx", "gy"), None, None),
        ),
        out_specs=P(("gx", "gy"), None, None),
        check_vma=False,
    )
```

```python
import jax
import jax.numpy as jnp
from jax import lax
from jax.experimental import pallas as pl
from jax.experimental.pallas import tpu as pltpu
from jax.sharding import PartitionSpec as P

MESH = pl.DeviceIdType.MESH
BF16 = jnp.bfloat16
F32 = jnp.float32


def turned(x):
    lane = lax.broadcasted_iota(jnp.int32, (1, 128), 1)
    return pltpu.roll(x, 64, 1) * jnp.where(lane < 64, -1.0, 1.0).astype(BF16)


def dot(a, b):
    return jnp.dot(a, b, preferred_element_type=F32).astype(BF16)


def mixed(own, partner, transfer):
    operand = jnp.concatenate([own, turned(own), partner, turned(partner)], axis=0)
    return dot(transfer, operand)


def mixed_pair(a, b, transfer_a, transfer_b):
    operand = jnp.concatenate([a, turned(a), b, turned(b)], axis=0)
    out = dot(jnp.concatenate([transfer_a, pltpu.roll(transfer_b, 64, 1)], axis=0), operand)
    return out[:32], out[32:]


def paired(values, bit, transfer):
    result = [None] * len(values)
    for n in range(len(values)):
        if n < n ^ bit:
            m = n ^ bit
            result[n], result[m] = mixed_pair(values[n], values[m], transfer(n), transfer(m))
    return result


NH = 8
CH = 8 // NH
LAG = 6


def kernel(
    src, leaf, st, tt, out,
    src_v, leaf_v, s0, sb, sq, z3, t01, t23, c0, c0p, c1, cb, yk, ys, yp, wm, mb, rb,
    load_sem, own_sem, s_recv, s3_recv, z3_recv, t_recv, p_recv, y_recv, z_recv, m_recv, r_recv, sent,
):
    x = lax.axis_index("gx")
    g = lax.axis_index("gy")
    z = g // 8
    z1 = z // 2
    z0 = z % 2
    a = (z0 + z1) % 2
    other = 1 - a
    yc = g % 8
    core = g % 2
    mate = z + 1 - 2 * z0

    def z_of(a_bit, k):
        return 2 * k + (a_bit + k) % 2

    def remote(source, target, send, recv, device):
        return pltpu.make_async_remote_copy(
            src_ref=source,
            dst_ref=target,
            send_sem=sent.at[send],
            recv_sem=recv,
            device_id=device,
            device_id_type=MESH,
        )

    def drain(ref, sem):
        pltpu.make_async_copy(ref, ref, sem).wait()

    def s_copy(k, r):
        to = (yc + r) % 8
        return remote(
            st.at[pl.ds(1, 2), :, k, :, to], sb.at[:, yc, k], 0, s_recv.at[k], (x, z * 8 + to)
        )

    def s3_copy(k, r):
        to = (yc + r) % 8
        return remote(
            st.at[3, :, k, (a + k) % 2, to], sq.at[yc, k], 1, s3_recv.at[k], (x, z * 8 + to)
        )

    def cross_copy(k):
        return remote(
            st.at[3, :, k, (other + k) % 2], z3.at[k], 9, z3_recv.at[k], (x, mate * 8 + yc)
        )

    def pass_copy(k, r):
        to = (yc + r) % 8
        return remote(
            z3.at[k, :, to], sq.at[8 + yc, k], 1, s3_recv.at[k], (x, z * 8 + to)
        )

    def t01_copy(i, h):
        to_x = (x + i) % 4
        to_z1 = (z1 + h) % 2
        return remote(
            tt.at[pl.ds(0, 2), to_x, to_z1],
            t01.at[:, 2 * x + z1],
            2,
            t_recv.at[0],
            (to_x, z_of(a, to_z1) * 8 + yc),
        )

    def t23_copy(level, to_z):
        return remote(
            tt.at[level + 2, :, to_z // 2, to_z % 2],
            t23.at[level, z],
            3,
            t_recv.at[1 + level],
            (x, to_z * 8 + yc),
        )

    def p_copy(k):
        return remote(c0.at[k], c0p.at[k], 4, p_recv.at[k], (x, g + 1 - 2 * core))

    def y_copy(k, r):
        to = (yc + r) % 8
        return remote(c1.at[to, k], cb.at[yc, k], 5, y_recv.at[k], (x, z * 8 + to))

    def z_copy(k, q):
        chunk = pl.ds(CH * q, CH)
        return remote(
            ys.at[k, chunk], yp.at[k, chunk], 6, z_recv.at[k, q], (x, mate * 8 + yc)
        )

    def m_copy(k, q, i, h):
        chunk = pl.ds(CH * q, CH)
        to_x = (x + i) % 4
        to_z0 = (z0 + h) % 2
        return remote(
            wm.at[to_z0, to_x, k, chunk],
            mb.at[2 * x + a, k, chunk],
            7,
            m_recv.at[q],
            (to_x, (2 * z1 + to_z0) * 8 + yc),
        )

    def r_copy(q, to_z):
        chunk = pl.ds(CH * q, CH)
        return remote(
            rb.at[to_z, :, chunk], out.at[:, z, chunk], 8, r_recv, (x, to_z * 8 + yc)
        )

    near = [(i, h) for h in range(2) for i in (1, 3, 2, 0) if (i, h) != (0, 0)]
    along_y = [2, 6, 4, 1, 3, 7, 5]
    along_z = [mate, (z + 2) % 4, (mate + 2) % 4]

    loads = [
        pltpu.make_async_copy(src, src_v, load_sem.at[0]),
        pltpu.make_async_copy(leaf, leaf_v, load_sem.at[1]),
        pltpu.make_async_copy(st.at[0], s0, load_sem.at[2]),
    ]
    for copy in loads:
        copy.start()
    own_s = [
        pltpu.make_async_copy(st.at[pl.ds(1, 2), :, k, :, yc], sb.at[:, yc, k], own_sem.at[k])
        for k in range(2)
    ]
    own_s3 = [
        pltpu.make_async_copy(st.at[3, :, k, (a + k) % 2, yc], sq.at[yc, k], own_sem.at[2 + k])
        for k in range(2)
    ]
    own_t01 = pltpu.make_async_copy(tt.at[pl.ds(0, 2), x, z1], t01.at[:, 2 * x + z1], own_sem.at[4])
    own_t23 = pltpu.make_async_copy(tt.at[pl.ds(2, 2), :, z1, z0], t23.at[:, z], own_sem.at[5])
    for copy in own_s + own_s3 + [own_t01, own_t23]:
        copy.start()

    barrier = pltpu.get_barrier_semaphore()
    peers = [(x, z * 8 + (yc + r) % 8) for r in range(1, 8)]
    peers += [(x, ((z + j) % 4) * 8 + yc) for j in range(1, 4)]
    for i in range(1, 4):
        for to_z in (z, mate, z_of(a, 1 - z1)):
            peers.append(((x + i) % 4, to_z * 8 + yc))
    for peer in peers:
        pl.semaphore_signal(barrier, inc=1, device_id=peer, device_id_type=MESH)

    pl.semaphore_wait(barrier, len(peers))
    for r in along_y:
        s_copy(0, r).start()
    for k in range(2):
        cross_copy(k).start()
    for i, h in near:
        t01_copy(i, h).start()
    for level in range(2):
        t23_copy(level, mate).start()

    loads[0].wait()
    loads[1].wait()
    for k in range(2):

        def leaf_body(n, carry, k=k):
            for w in range(4):
                vx, j = 2 * n + w // 2, w % 2
                for i in range(8):
                    v = src_v[vx, k, j, i]
                    c0[k, vx, j, i] = dot(
                        leaf_v[vx, k, j, i], jnp.concatenate([v, turned(v)], axis=0)
                    )
            return carry

        lax.fori_loop(0, 2, leaf_body, 0)
        p_copy(k).start()

    def last_source(k):
        for r in along_y:
            s3_copy(k, r).start()
        drain(z3.at[k], z3_recv.at[k])
        for r in along_y:
            pass_copy(k, r).start()
        sq[8 + yc, k] = z3[k, :, yc]

    loads[2].wait()
    for k in range(2):
        p_copy(k).wait_recv()

        def first_body(n, carry, k=k):
            for w in range(4):
                vx, j = 2 * n + w // 2, w % 2
                for i in range(8):
                    c1[i, k, vx, j] = mixed(c0[k, vx, j, i], c0p[k, vx, j, i], s0[vx, k, j, i])
            return carry

        lax.fori_loop(0, 2, first_body, 0)
        for r in along_y:
            y_copy(k, r).start()
        if k == 0:
            last_source(0)
            for r in along_y:
                s_copy(1, r).start()
        cb[yc, k] = c1[yc, k]

    sides = (z0, 1 - z0)

    def x_stage(k, q):
        z_copy(k, q).wait_recv()

        rows = [CH * q + b for b in range(CH)]
        values = [v for i in rows for m in (yk, yp) for v in [m[k, i, n] for n in range(4)]]
        values = paired(
            values, 4, lambda n: sq[8 * (n // 4 % 2) + rows[n // 8], k, n % 4]
        )
        for level, bit in enumerate((2, 1)):
            values = paired(
                values,
                bit,
                lambda n: t01[level, 2 * (n % 4) + k, sides[n // 4 % 2], rows[n // 8]],
            )
        for n in range(8 * CH):
            wm[sides[n // 4 % 2], n % 4, k, rows[n // 8]] = values[n]
        for i, h in near:
            m_copy(k, q, i, h).start()
        chunk = pl.ds(CH * q, CH)
        mb[2 * x + a, k, chunk] = wm[z0, x, k, chunk]

    def last_stage(q):
        drain(mb.at[pl.ds(0, 7), :, pl.ds(CH * q, CH)], m_recv.at[q])

        places = [(CH * q + b, n) for b in range(CH) for n in range(4)]
        values = [mb[2 * n + m // 2, m % 2, i] for i, n in places for m in range(4)]
        for level, bit in enumerate((3, 2)):
            values = paired(
                values,
                bit,
                lambda w: t23[
                    level, z_of(w % 4 // 2, w % 2), places[w // 4][1], places[w // 4][0]
                ],
            )
        for w in range(len(values)):
            rb[z_of(w % 4 // 2, w % 2), places[w // 4][1], places[w // 4][0]] = values[w]
        for to_z in along_z:
            r_copy(q, to_z).start()
        chunk = pl.ds(CH * q, CH)
        out[:, z, chunk] = rb[z, :, chunk]

    for k in range(2):
        own_s[k].wait()
        drain(sb.at[:, pl.ds(0, 7), k], s_recv.at[k])
        drain(cb.at[pl.ds(0, 7), k], y_recv.at[k])

        def y_body(h, carry, k=k):
            columns = [
                (2 * h + n, target, (a_bit + k) % 2)
                for n in range(2)
                for target, a_bit in ((ys, other), (yk, a))
            ]
            values = [cb[i, k, vx, j] for vx, _, j in columns for i in range(8)]
            for level, bit in enumerate((2, 4)):
                values = paired(
                    values,
                    bit,
                    lambda n: sb[level, n % 8, k, columns[n // 8][0], columns[n // 8][2]],
                )
            for n in range(32):
                vx, target, _ = columns[n // 8]
                target[k, n % 8, vx] = values[n]
            return carry

        lax.fori_loop(0, 2, y_body, 0)
        for q in range(NH):
            z_copy(k, q).start()
        if k == 0:
            last_source(1)
            for level in range(2):
                for to_z in along_z[1:]:
                    t23_copy(level, to_z).start()

        own_s3[k].wait()
        drain(sq.at[pl.ds(0, 14), k], s3_recv.at[k])
        if k == 0:
            own_t01.wait()
            drain(t01.at[:, pl.ds(0, 7)], t_recv.at[0])
            for q in range(NH):
                x_stage(0, q)

    own_t23.wait()
    for q in range(NH + LAG):
        if q < NH:
            x_stage(1, q)
        if q == LAG:
            for level in range(2):
                drain(t23.at[level, pl.ds(0, 3)], t_recv.at[1 + level])
        if q >= LAG:
            last_stage(q - LAG)

    drain(out.at[:, pl.ds(0, 3)], r_recv)
    drain(sb.at[:, pl.ds(0, 7)], sent.at[0])
    drain(sq.at[pl.ds(0, 14)], sent.at[1])
    drain(z3, sent.at[9])
    drain(t01.at[:, pl.ds(0, 7)], sent.at[2])
    drain(t23.at[:, pl.ds(0, 3)], sent.at[3])
    drain(c0, sent.at[4])
    drain(cb.at[pl.ds(0, 7)], sent.at[5])
    drain(ys, sent.at[6])
    drain(mb.at[pl.ds(0, 7)], sent.at[7])
    drain(out.at[:, pl.ds(0, 3)], sent.at[8])


def local(source_values, leaf_maps, source_transfers, target_transfers):
    dma = pltpu.SemaphoreType.DMA
    box = (32, 128)

    def vmem(*shape):
        return pltpu.VMEM(shape + box, BF16)

    out = pl.pallas_call(
        kernel,
        out_shape=jax.ShapeDtypeStruct((4, 4, 8) + box, BF16),
        in_specs=[pl.BlockSpec(memory_space=pl.ANY)] * 4,
        out_specs=pl.BlockSpec(memory_space=pltpu.VMEM),
        scratch_shapes=[
            pltpu.VMEM((4, 2, 2, 8, 64, 128), BF16),
            vmem(4, 2, 2, 8),
            vmem(4, 2, 2, 8),
            vmem(2, 8, 2, 4, 2),
            vmem(16, 2, 4),
            vmem(2, 4, 8),
            vmem(2, 8, 2, 8),
            vmem(2, 4, 4, 8),
            vmem(2, 4, 2, 8),
            vmem(2, 4, 2, 8),
            vmem(8, 2, 4, 2),
            vmem(8, 2, 4, 2),
            vmem(2, 8, 4),
            vmem(2, 8, 4),
            vmem(2, 8, 4),
            vmem(2, 4, 2, 8),
            vmem(8, 2, 8),
            vmem(4, 4, 8),
            dma((3,)),
            dma((6,)),
            dma((2,)),
            dma((2,)),
            dma((2,)),
            dma((3,)),
            dma((2,)),
            dma((2,)),
            dma((2, NH)),
            dma((NH,)),
            dma,
            dma((10,)),
        ],
        compiler_params=pltpu.CompilerParams(
            collective_id=0, has_side_effects=True, vmem_limit_bytes=54000 * 1024
        ),
    )(
        source_values.reshape(4, 2, 2, 8, 64, 128),
        leaf_maps.reshape((4, 2, 2, 8) + box),
        source_transfers.reshape((4, 4, 2, 2, 8) + box),
        target_transfers.reshape((4, 4, 2, 2, 8) + box),
    )
    return out.reshape((128,) + box)


def solution(mesh):
    return jax.shard_map(
        local,
        mesh=mesh,
        in_specs=(
            P(("gx", "gy"), None, None),
            P(("gx", "gy"), None, None),
            P(None, ("gx", "gy"), None, None),
            P(None, ("gx", "gy"), None, None),
        ),
        out_specs=P(("gx", "gy"), None, None),
        check_vma=False,
    )
```

```python
import jax
import jax.numpy as jnp
from jax import lax
from jax.experimental import pallas as pl
from jax.experimental.pallas import tpu as pltpu
from jax.sharding import PartitionSpec as P

MESH = pl.DeviceIdType.MESH
BF16 = jnp.bfloat16
F32 = jnp.float32


def turned(x):
    lane = lax.broadcasted_iota(jnp.int32, (1, 128), 1)
    return pltpu.roll(x, 64, 1) * jnp.where(lane < 64, -1.0, 1.0).astype(BF16)


def dot(a, b):
    return jnp.dot(a, b, preferred_element_type=F32).astype(BF16)


def mixed(own, partner, transfer):
    operand = jnp.concatenate([own, turned(own), partner, turned(partner)], axis=0)
    return dot(transfer, operand)


def mixed_pair(a, b, transfer_a, transfer_b):
    operand = jnp.concatenate([a, turned(a), b, turned(b)], axis=0)
    out = dot(jnp.concatenate([transfer_a, pltpu.roll(transfer_b, 64, 1)], axis=0), operand)
    return out[:32], out[32:]


def paired(values, bit, transfer):
    result = [None] * len(values)
    for n in range(len(values)):
        if n < n ^ bit:
            m = n ^ bit
            result[n], result[m] = mixed_pair(values[n], values[m], transfer(n), transfer(m))
    return result


NH = 8
CH = 8 // NH
LAG = 6


def kernel(
    src, leaf, st, tt, out,
    src_v, leaf_v, s0, sb, sq, z3, t01, t23, c0, c0p, c1, cb, yk, ys, yp, wm, mb, rb,
    load_sem, own_sem, s_recv, s3_recv, z3_recv, t_recv, p_recv, y_recv, z_recv, m_recv, r_recv, sent,
):
    x = lax.axis_index("gx")
    g = lax.axis_index("gy")
    z = g // 8
    z1 = z // 2
    z0 = z % 2
    a = (z0 + z1) % 2
    other = 1 - a
    yc = g % 8
    core = g % 2
    mate = z + 1 - 2 * z0

    def z_of(a_bit, k):
        return 2 * k + (a_bit + k) % 2

    def remote(source, target, send, recv, device):
        return pltpu.make_async_remote_copy(
            src_ref=source,
            dst_ref=target,
            send_sem=sent.at[send],
            recv_sem=recv,
            device_id=device,
            device_id_type=MESH,
        )

    def drain(ref, sem):
        pltpu.make_async_copy(ref, ref, sem).wait()

    def s_copy(k, r):
        to = (yc + r) % 8
        return remote(
            st.at[pl.ds(1, 2), :, k, :, to], sb.at[:, yc, k], 0, s_recv.at[k], (x, z * 8 + to)
        )

    def s3_copy(k, r):
        to = (yc + r) % 8
        return remote(
            st.at[3, :, k, (a + k) % 2, to], sq.at[yc, k], 1, s3_recv.at[k], (x, z * 8 + to)
        )

    def cross_copy(k):
        return remote(
            st.at[3, :, k, (other + k) % 2], z3.at[k], 9, z3_recv.at[k], (x, mate * 8 + yc)
        )

    def pass_copy(k, r):
        to = (yc + r) % 8
        return remote(
            z3.at[k, :, to], sq.at[8 + yc, k], 1, s3_recv.at[k], (x, z * 8 + to)
        )

    def t01_copy(i, h):
        to_x = (x + i) % 4
        to_z1 = (z1 + h) % 2
        return remote(
            tt.at[pl.ds(0, 2), to_x, to_z1],
            t01.at[:, 2 * x + z1],
            2,
            t_recv.at[0],
            (to_x, z_of(a, to_z1) * 8 + yc),
        )

    def t23_copy(level, to_z):
        return remote(
            tt.at[level + 2, :, to_z // 2, to_z % 2],
            t23.at[level, z],
            3,
            t_recv.at[1 + level],
            (x, to_z * 8 + yc),
        )

    def p_copy(k):
        return remote(c0.at[k], c0p.at[k], 4, p_recv.at[k], (x, g + 1 - 2 * core))

    def y_copy(k, r):
        to = (yc + r) % 8
        return remote(c1.at[to, k], cb.at[yc, k], 5, y_recv.at[k], (x, z * 8 + to))

    def z_copy(k, q):
        chunk = pl.ds(CH * q, CH)
        return remote(
            ys.at[k, chunk], yp.at[k, chunk], 6, z_recv.at[k, q], (x, mate * 8 + yc)
        )

    def m_copy(k, q, i, h):
        chunk = pl.ds(CH * q, CH)
        to_x = (x + i) % 4
        to_z0 = (z0 + h) % 2
        return remote(
            wm.at[to_z0, to_x, k, chunk],
            mb.at[2 * x + a, k, chunk],
            7,
            m_recv.at[q],
            (to_x, (2 * z1 + to_z0) * 8 + yc),
        )

    def r_copy(q, to_z):
        chunk = pl.ds(CH * q, CH)
        return remote(
            rb.at[to_z, :, chunk], out.at[:, z, chunk], 8, r_recv, (x, to_z * 8 + yc)
        )

    near = [(i, h) for h in range(2) for i in (1, 3, 2, 0) if (i, h) != (0, 0)]
    along_y = [4, 3, 5, 2, 6, 1, 7]
    along_z = [mate, (z + 2) % 4, (mate + 2) % 4]

    loads = [
        pltpu.make_async_copy(src, src_v, load_sem.at[0]),
        pltpu.make_async_copy(leaf, leaf_v, load_sem.at[1]),
        pltpu.make_async_copy(st.at[0], s0, load_sem.at[2]),
    ]
    for copy in loads:
        copy.start()
    own_s = [
        pltpu.make_async_copy(st.at[pl.ds(1, 2), :, k, :, yc], sb.at[:, yc, k], own_sem.at[k])
        for k in range(2)
    ]
    own_s3 = [
        pltpu.make_async_copy(st.at[3, :, k, (a + k) % 2, yc], sq.at[yc, k], own_sem.at[2 + k])
        for k in range(2)
    ]
    own_t01 = pltpu.make_async_copy(tt.at[pl.ds(0, 2), x, z1], t01.at[:, 2 * x + z1], own_sem.at[4])
    own_t23 = pltpu.make_async_copy(tt.at[pl.ds(2, 2), :, z1, z0], t23.at[:, z], own_sem.at[5])
    for copy in own_s + own_s3 + [own_t01, own_t23]:
        copy.start()

    barrier = pltpu.get_barrier_semaphore()
    peers = [(x, z * 8 + (yc + r) % 8) for r in range(1, 8)]
    peers += [(x, ((z + j) % 4) * 8 + yc) for j in range(1, 4)]
    for i in range(1, 4):
        for to_z in (z, mate, z_of(a, 1 - z1)):
            peers.append(((x + i) % 4, to_z * 8 + yc))
    for peer in peers:
        pl.semaphore_signal(barrier, inc=1, device_id=peer, device_id_type=MESH)

    pl.semaphore_wait(barrier, len(peers))
    for r in along_y:
        s_copy(0, r).start()
    for k in range(2):
        cross_copy(k).start()
    for i, h in near:
        t01_copy(i, h).start()
    for level in range(2):
        t23_copy(level, mate).start()

    loads[0].wait()
    loads[1].wait()
    for k in range(2):

        def leaf_body(n, carry, k=k):
            for w in range(4):
                vx, j = 2 * n + w // 2, w % 2
                for i in range(8):
                    v = src_v[vx, k, j, i]
                    c0[k, vx, j, i] = dot(
                        leaf_v[vx, k, j, i], jnp.concatenate([v, turned(v)], axis=0)
                    )
            return carry

        lax.fori_loop(0, 2, leaf_body, 0)
        p_copy(k).start()

    def last_source(k):
        for r in along_y:
            s3_copy(k, r).start()
        drain(z3.at[k], z3_recv.at[k])
        for r in along_y:
            pass_copy(k, r).start()
        sq[8 + yc, k] = z3[k, :, yc]

    loads[2].wait()
    for k in range(2):
        p_copy(k).wait_recv()

        def first_body(n, carry, k=k):
            for w in range(4):
                vx, j = 2 * n + w // 2, w % 2
                for i in range(8):
                    c1[i, k, vx, j] = mixed(c0[k, vx, j, i], c0p[k, vx, j, i], s0[vx, k, j, i])
            return carry

        lax.fori_loop(0, 2, first_body, 0)
        for r in along_y:
            y_copy(k, r).start()
        if k == 0:
            last_source(0)
            for r in along_y:
                s_copy(1, r).start()
        cb[yc, k] = c1[yc, k]

    sides = (z0, 1 - z0)

    def x_stage(k, q):
        z_copy(k, q).wait_recv()

        rows = [CH * q + b for b in range(CH)]
        values = [v for i in rows for m in (yk, yp) for v in [m[k, i, n] for n in range(4)]]
        values = paired(
            values, 4, lambda n: sq[8 * (n // 4 % 2) + rows[n // 8], k, n % 4]
        )
        for level, bit in enumerate((2, 1)):
            values = paired(
                values,
                bit,
                lambda n: t01[level, 2 * (n % 4) + k, sides[n // 4 % 2], rows[n // 8]],
            )
        for n in range(8 * CH):
            wm[sides[n // 4 % 2], n % 4, k, rows[n // 8]] = values[n]
        for i, h in near:
            m_copy(k, q, i, h).start()
        chunk = pl.ds(CH * q, CH)
        mb[2 * x + a, k, chunk] = wm[z0, x, k, chunk]

    def last_stage(q):
        drain(mb.at[pl.ds(0, 7), :, pl.ds(CH * q, CH)], m_recv.at[q])

        places = [(CH * q + b, n) for b in range(CH) for n in range(4)]
        values = [mb[2 * n + m // 2, m % 2, i] for i, n in places for m in range(4)]
        for level, bit in enumerate((3, 2)):
            values = paired(
                values,
                bit,
                lambda w: t23[
                    level, z_of(w % 4 // 2, w % 2), places[w // 4][1], places[w // 4][0]
                ],
            )
        for w in range(len(values)):
            rb[z_of(w % 4 // 2, w % 2), places[w // 4][1], places[w // 4][0]] = values[w]
        for to_z in along_z:
            r_copy(q, to_z).start()
        chunk = pl.ds(CH * q, CH)
        out[:, z, chunk] = rb[z, :, chunk]

    for k in range(2):
        own_s[k].wait()
        drain(sb.at[:, pl.ds(0, 7), k], s_recv.at[k])
        drain(cb.at[pl.ds(0, 7), k], y_recv.at[k])

        def y_body(h, carry, k=k):
            columns = [
                (2 * h + n, target, (a_bit + k) % 2)
                for n in range(2)
                for target, a_bit in ((ys, other), (yk, a))
            ]
            values = [cb[i, k, vx, j] for vx, _, j in columns for i in range(8)]
            for level, bit in enumerate((2, 4)):
                values = paired(
                    values,
                    bit,
                    lambda n: sb[level, n % 8, k, columns[n // 8][0], columns[n // 8][2]],
                )
            for n in range(32):
                vx, target, _ = columns[n // 8]
                target[k, n % 8, vx] = values[n]
            return carry

        lax.fori_loop(0, 2, y_body, 0)
        for q in range(NH):
            z_copy(k, q).start()
        if k == 0:
            last_source(1)
            for level in range(2):
                for to_z in along_z[1:]:
                    t23_copy(level, to_z).start()

        own_s3[k].wait()
        drain(sq.at[pl.ds(0, 14), k], s3_recv.at[k])
        if k == 0:
            own_t01.wait()
            drain(t01.at[:, pl.ds(0, 7)], t_recv.at[0])
            for q in range(NH):
                x_stage(0, q)

    own_t23.wait()
    for q in range(NH + LAG):
        if q < NH:
            x_stage(1, q)
        if q == LAG:
            for level in range(2):
                drain(t23.at[level, pl.ds(0, 3)], t_recv.at[1 + level])
        if q >= LAG:
            last_stage(q - LAG)

    drain(out.at[:, pl.ds(0, 3)], r_recv)
    drain(sb.at[:, pl.ds(0, 7)], sent.at[0])
    drain(sq.at[pl.ds(0, 14)], sent.at[1])
    drain(z3, sent.at[9])
    drain(t01.at[:, pl.ds(0, 7)], sent.at[2])
    drain(t23.at[:, pl.ds(0, 3)], sent.at[3])
    drain(c0, sent.at[4])
    drain(cb.at[pl.ds(0, 7)], sent.at[5])
    drain(ys, sent.at[6])
    drain(mb.at[pl.ds(0, 7)], sent.at[7])
    drain(out.at[:, pl.ds(0, 3)], sent.at[8])


def local(source_values, leaf_maps, source_transfers, target_transfers):
    dma = pltpu.SemaphoreType.DMA
    box = (32, 128)

    def vmem(*shape):
        return pltpu.VMEM(shape + box, BF16)

    out = pl.pallas_call(
        kernel,
        out_shape=jax.ShapeDtypeStruct((4, 4, 8) + box, BF16),
        in_specs=[pl.BlockSpec(memory_space=pl.ANY)] * 4,
        out_specs=pl.BlockSpec(memory_space=pltpu.VMEM),
        scratch_shapes=[
            pltpu.VMEM((4, 2, 2, 8, 64, 128), BF16),
            vmem(4, 2, 2, 8),
            vmem(4, 2, 2, 8),
            vmem(2, 8, 2, 4, 2),
            vmem(16, 2, 4),
            vmem(2, 4, 8),
            vmem(2, 8, 2, 8),
            vmem(2, 4, 4, 8),
            vmem(2, 4, 2, 8),
            vmem(2, 4, 2, 8),
            vmem(8, 2, 4, 2),
            vmem(8, 2, 4, 2),
            vmem(2, 8, 4),
            vmem(2, 8, 4),
            vmem(2, 8, 4),
            vmem(2, 4, 2, 8),
            vmem(8, 2, 8),
            vmem(4, 4, 8),
            dma((3,)),
            dma((6,)),
            dma((2,)),
            dma((2,)),
            dma((2,)),
            dma((3,)),
            dma((2,)),
            dma((2,)),
            dma((2, NH)),
            dma((NH,)),
            dma,
            dma((10,)),
        ],
        compiler_params=pltpu.CompilerParams(
            collective_id=0, has_side_effects=True, vmem_limit_bytes=54000 * 1024
        ),
    )(
        source_values.reshape(4, 2, 2, 8, 64, 128),
        leaf_maps.reshape((4, 2, 2, 8) + box),
        source_transfers.reshape((4, 4, 2, 2, 8) + box),
        target_transfers.reshape((4, 4, 2, 2, 8) + box),
    )
    return out.reshape((128,) + box)


def solution(mesh):
    return jax.shard_map(
        local,
        mesh=mesh,
        in_specs=(
            P(("gx", "gy"), None, None),
            P(("gx", "gy"), None, None),
            P(None, ("gx", "gy"), None, None),
            P(None, ("gx", "gy"), None, None),
        ),
        out_specs=P(("gx", "gy"), None, None),
        check_vma=False,
    )
```

```python
import jax
import jax.numpy as jnp
from jax import lax
from jax.experimental import pallas as pl
from jax.experimental.pallas import tpu as pltpu
from jax.sharding import PartitionSpec as P

MESH = pl.DeviceIdType.MESH
BF16 = jnp.bfloat16
F32 = jnp.float32


def turned(x):
    lane = lax.broadcasted_iota(jnp.int32, (1, 128), 1)
    return pltpu.roll(x, 64, 1) * jnp.where(lane < 64, -1.0, 1.0).astype(BF16)


def dot(a, b):
    return jnp.dot(a, b, preferred_element_type=F32).astype(BF16)


def mixed(own, partner, transfer):
    operand = jnp.concatenate([own, turned(own), partner, turned(partner)], axis=0)
    return dot(transfer, operand)


def mixed_pair(a, b, transfer_a, transfer_b):
    operand = jnp.concatenate([a, turned(a), b, turned(b)], axis=0)
    out = dot(jnp.concatenate([transfer_a, pltpu.roll(transfer_b, 64, 1)], axis=0), operand)
    return out[:32], out[32:]


def paired(values, bit, transfer):
    result = [None] * len(values)
    for n in range(len(values)):
        if n < n ^ bit:
            m = n ^ bit
            result[n], result[m] = mixed_pair(values[n], values[m], transfer(n), transfer(m))
    return result


NH = 8
CH = 8 // NH
LAG = 6


def kernel(
    src, leaf, st, tt, out,
    src_v, leaf_v, s0, sb, sq, z3, t01, t23, c0, c0p, c1, cb, yk, ys, yp, wm, mb, rb,
    load_sem, own_sem, s_recv, s3_recv, z3_recv, t_recv, p_recv, y_recv, z_recv, m_recv, r_recv, sent,
):
    x = lax.axis_index("gx")
    g = lax.axis_index("gy")
    z = g // 8
    z1 = z // 2
    z0 = z % 2
    a = (z0 + z1) % 2
    other = 1 - a
    yc = g % 8
    core = g % 2
    mate = z + 1 - 2 * z0

    def z_of(a_bit, k):
        return 2 * k + (a_bit + k) % 2

    def remote(source, target, send, recv, device):
        return pltpu.make_async_remote_copy(
            src_ref=source,
            dst_ref=target,
            send_sem=sent.at[send],
            recv_sem=recv,
            device_id=device,
            device_id_type=MESH,
        )

    def drain(ref, sem):
        pltpu.make_async_copy(ref, ref, sem).wait()

    def s_copy(k, r):
        to = (yc + r) % 8
        return remote(
            st.at[pl.ds(1, 2), :, k, :, to], sb.at[:, yc, k], 0, s_recv.at[k], (x, z * 8 + to)
        )

    def s3_copy(k, r):
        to = (yc + r) % 8
        return remote(
            st.at[3, :, k, (a + k) % 2, to], sq.at[yc, k], 1, s3_recv.at[k], (x, z * 8 + to)
        )

    def cross_copy(k):
        return remote(
            st.at[3, :, k, (other + k) % 2], z3.at[k], 9, z3_recv.at[k], (x, mate * 8 + yc)
        )

    def pass_copy(k, r):
        to = (yc + r) % 8
        return remote(
            z3.at[k, :, to], sq.at[8 + yc, k], 1, s3_recv.at[k], (x, z * 8 + to)
        )

    def t01_copy(i, h):
        to_x = (x + i) % 4
        to_z1 = (z1 + h) % 2
        return remote(
            tt.at[pl.ds(0, 2), to_x, to_z1],
            t01.at[:, 2 * x + z1],
            2,
            t_recv.at[0],
            (to_x, z_of(a, to_z1) * 8 + yc),
        )

    def t23_copy(level, to_z):
        return remote(
            tt.at[level + 2, :, to_z // 2, to_z % 2],
            t23.at[level, z],
            3,
            t_recv.at[1 + level],
            (x, to_z * 8 + yc),
        )

    def p_copy(k):
        return remote(c0.at[k], c0p.at[k], 4, p_recv.at[k], (x, g + 1 - 2 * core))

    def y_copy(k, r):
        to = (yc + r) % 8
        return remote(c1.at[to, k], cb.at[yc, k], 5, y_recv.at[k], (x, z * 8 + to))

    def z_copy(k, q):
        chunk = pl.ds(CH * q, CH)
        return remote(
            ys.at[k, chunk], yp.at[k, chunk], 6, z_recv.at[k, q], (x, mate * 8 + yc)
        )

    def m_copy(k, q, i, h):
        chunk = pl.ds(CH * q, CH)
        to_x = (x + i) % 4
        to_z0 = (z0 + h) % 2
        return remote(
            wm.at[to_z0, to_x, k, chunk],
            mb.at[2 * x + a, k, chunk],
            7,
            m_recv.at[q],
            (to_x, (2 * z1 + to_z0) * 8 + yc),
        )

    def r_copy(q, to_z):
        chunk = pl.ds(CH * q, CH)
        return remote(
            rb.at[to_z, :, chunk], out.at[:, z, chunk], 8, r_recv, (x, to_z * 8 + yc)
        )

    near = [(i, h) for h in range(2) for i in (1, 3, 2, 0) if (i, h) != (0, 0)]
    along_y = [4, 3, 5, 2, 6, 1, 7]
    along_z = [mate, (z + 2) % 4, (mate + 2) % 4]

    loads = [
        pltpu.make_async_copy(src, src_v, load_sem.at[0]),
        pltpu.make_async_copy(leaf, leaf_v, load_sem.at[1]),
        pltpu.make_async_copy(st.at[0], s0, load_sem.at[2]),
    ]
    for copy in loads:
        copy.start()
    own_s = [
        pltpu.make_async_copy(st.at[pl.ds(1, 2), :, k, :, yc], sb.at[:, yc, k], own_sem.at[k])
        for k in range(2)
    ]
    own_s3 = [
        pltpu.make_async_copy(st.at[3, :, k, (a + k) % 2, yc], sq.at[yc, k], own_sem.at[2 + k])
        for k in range(2)
    ]
    own_t01 = pltpu.make_async_copy(tt.at[pl.ds(0, 2), x, z1], t01.at[:, 2 * x + z1], own_sem.at[4])
    own_t23 = pltpu.make_async_copy(tt.at[pl.ds(2, 2), :, z1, z0], t23.at[:, z], own_sem.at[5])
    for copy in own_s + own_s3 + [own_t01, own_t23]:
        copy.start()

    barrier = pltpu.get_barrier_semaphore()
    peers = [(x, z * 8 + (yc + r) % 8) for r in range(1, 8)]
    peers += [(x, ((z + j) % 4) * 8 + yc) for j in range(1, 4)]
    for i in range(1, 4):
        for to_z in (z, mate, z_of(a, 1 - z1)):
            peers.append(((x + i) % 4, to_z * 8 + yc))
    for peer in peers[::-1]:
        pl.semaphore_signal(barrier, inc=1, device_id=peer, device_id_type=MESH)

    pl.semaphore_wait(barrier, len(peers))
    for r in along_y:
        s_copy(0, r).start()
    for k in range(2):
        cross_copy(k).start()
    for i, h in near:
        t01_copy(i, h).start()
    for level in range(2):
        t23_copy(level, mate).start()

    loads[0].wait()
    loads[1].wait()
    for k in range(2):

        def leaf_body(n, carry, k=k):
            for w in range(4):
                vx, j = 2 * n + w // 2, w % 2
                for i in range(8):
                    v = src_v[vx, k, j, i]
                    c0[k, vx, j, i] = dot(
                        leaf_v[vx, k, j, i], jnp.concatenate([v, turned(v)], axis=0)
                    )
            return carry

        lax.fori_loop(0, 2, leaf_body, 0)
        p_copy(k).start()

    def last_source(k):
        for r in along_y:
            s3_copy(k, r).start()
        drain(z3.at[k], z3_recv.at[k])
        for r in along_y:
            pass_copy(k, r).start()
        sq[8 + yc, k] = z3[k, :, yc]

    loads[2].wait()
    for k in range(2):
        p_copy(k).wait_recv()

        def first_body(n, carry, k=k):
            for w in range(4):
                vx, j = 2 * n + w // 2, w % 2
                for i in range(8):
                    c1[i, k, vx, j] = mixed(c0[k, vx, j, i], c0p[k, vx, j, i], s0[vx, k, j, i])
            return carry

        lax.fori_loop(0, 2, first_body, 0)
        for r in along_y:
            y_copy(k, r).start()
        if k == 0:
            last_source(0)
            for r in along_y:
                s_copy(1, r).start()
        cb[yc, k] = c1[yc, k]

    sides = (z0, 1 - z0)

    def x_stage(k, q):
        z_copy(k, q).wait_recv()

        rows = [CH * q + b for b in range(CH)]
        values = [v for i in rows for m in (yk, yp) for v in [m[k, i, n] for n in range(4)]]
        values = paired(
            values, 4, lambda n: sq[8 * (n // 4 % 2) + rows[n // 8], k, n % 4]
        )
        for level, bit in enumerate((2, 1)):
            values = paired(
                values,
                bit,
                lambda n: t01[level, 2 * (n % 4) + k, sides[n // 4 % 2], rows[n // 8]],
            )
        for n in range(8 * CH):
            wm[sides[n // 4 % 2], n % 4, k, rows[n // 8]] = values[n]
        for i, h in near:
            m_copy(k, q, i, h).start()
        chunk = pl.ds(CH * q, CH)
        mb[2 * x + a, k, chunk] = wm[z0, x, k, chunk]

    def last_stage(q):
        drain(mb.at[pl.ds(0, 7), :, pl.ds(CH * q, CH)], m_recv.at[q])

        places = [(CH * q + b, n) for b in range(CH) for n in range(4)]
        values = [mb[2 * n + m // 2, m % 2, i] for i, n in places for m in range(4)]
        for level, bit in enumerate((3, 2)):
            values = paired(
                values,
                bit,
                lambda w: t23[
                    level, z_of(w % 4 // 2, w % 2), places[w // 4][1], places[w // 4][0]
                ],
            )
        for w in range(len(values)):
            rb[z_of(w % 4 // 2, w % 2), places[w // 4][1], places[w // 4][0]] = values[w]
        for to_z in along_z:
            r_copy(q, to_z).start()
        chunk = pl.ds(CH * q, CH)
        out[:, z, chunk] = rb[z, :, chunk]

    for k in range(2):
        own_s[k].wait()
        drain(sb.at[:, pl.ds(0, 7), k], s_recv.at[k])
        drain(cb.at[pl.ds(0, 7), k], y_recv.at[k])

        def y_body(h, carry, k=k):
            columns = [
                (2 * h + n, target, (a_bit + k) % 2)
                for n in range(2)
                for target, a_bit in ((ys, other), (yk, a))
            ]
            values = [cb[i, k, vx, j] for vx, _, j in columns for i in range(8)]
            for level, bit in enumerate((2, 4)):
                values = paired(
                    values,
                    bit,
                    lambda n: sb[level, n % 8, k, columns[n // 8][0], columns[n // 8][2]],
                )
            for n in range(32):
                vx, target, _ = columns[n // 8]
                target[k, n % 8, vx] = values[n]
            return carry

        lax.fori_loop(0, 2, y_body, 0)
        for q in range(NH):
            z_copy(k, q).start()
        if k == 0:
            last_source(1)
            for level in range(2):
                for to_z in along_z[1:]:
                    t23_copy(level, to_z).start()

        own_s3[k].wait()
        drain(sq.at[pl.ds(0, 14), k], s3_recv.at[k])
        if k == 0:
            own_t01.wait()
            drain(t01.at[:, pl.ds(0, 7)], t_recv.at[0])
            for q in range(NH):
                x_stage(0, q)

    own_t23.wait()
    for q in range(NH + LAG):
        if q < NH:
            x_stage(1, q)
        if q == LAG:
            for level in range(2):
                drain(t23.at[level, pl.ds(0, 3)], t_recv.at[1 + level])
        if q >= LAG:
            last_stage(q - LAG)

    drain(out.at[:, pl.ds(0, 3)], r_recv)
    drain(sb.at[:, pl.ds(0, 7)], sent.at[0])
    drain(sq.at[pl.ds(0, 14)], sent.at[1])
    drain(z3, sent.at[9])
    drain(t01.at[:, pl.ds(0, 7)], sent.at[2])
    drain(t23.at[:, pl.ds(0, 3)], sent.at[3])
    drain(c0, sent.at[4])
    drain(cb.at[pl.ds(0, 7)], sent.at[5])
    drain(ys, sent.at[6])
    drain(mb.at[pl.ds(0, 7)], sent.at[7])
    drain(out.at[:, pl.ds(0, 3)], sent.at[8])


def local(source_values, leaf_maps, source_transfers, target_transfers):
    dma = pltpu.SemaphoreType.DMA
    box = (32, 128)

    def vmem(*shape):
        return pltpu.VMEM(shape + box, BF16)

    out = pl.pallas_call(
        kernel,
        out_shape=jax.ShapeDtypeStruct((4, 4, 8) + box, BF16),
        in_specs=[pl.BlockSpec(memory_space=pl.ANY)] * 4,
        out_specs=pl.BlockSpec(memory_space=pltpu.VMEM),
        scratch_shapes=[
            pltpu.VMEM((4, 2, 2, 8, 64, 128), BF16),
            vmem(4, 2, 2, 8),
            vmem(4, 2, 2, 8),
            vmem(2, 8, 2, 4, 2),
            vmem(16, 2, 4),
            vmem(2, 4, 8),
            vmem(2, 8, 2, 8),
            vmem(2, 4, 4, 8),
            vmem(2, 4, 2, 8),
            vmem(2, 4, 2, 8),
            vmem(8, 2, 4, 2),
            vmem(8, 2, 4, 2),
            vmem(2, 8, 4),
            vmem(2, 8, 4),
            vmem(2, 8, 4),
            vmem(2, 4, 2, 8),
            vmem(8, 2, 8),
            vmem(4, 4, 8),
            dma((3,)),
            dma((6,)),
            dma((2,)),
            dma((2,)),
            dma((2,)),
            dma((3,)),
            dma((2,)),
            dma((2,)),
            dma((2, NH)),
            dma((NH,)),
            dma,
            dma((10,)),
        ],
        compiler_params=pltpu.CompilerParams(
            collective_id=0, has_side_effects=True, vmem_limit_bytes=54000 * 1024
        ),
    )(
        source_values.reshape(4, 2, 2, 8, 64, 128),
        leaf_maps.reshape((4, 2, 2, 8) + box),
        source_transfers.reshape((4, 4, 2, 2, 8) + box),
        target_transfers.reshape((4, 4, 2, 2, 8) + box),
    )
    return out.reshape((128,) + box)


def solution(mesh):
    return jax.shard_map(
        local,
        mesh=mesh,
        in_specs=(
            P(("gx", "gy"), None, None),
            P(("gx", "gy"), None, None),
            P(None, ("gx", "gy"), None, None),
            P(None, ("gx", "gy"), None, None),
        ),
        out_specs=P(("gx", "gy"), None, None),
        check_vma=False,
    )
```
